32 devices in a mesh: row: 4 (over x, core), col: 8 (over z, y).
Axes of the slice: x: 2, y: 2, z: 4, core: 2. Of those that a mesh axis runs over, the one named last changes fastest.
Arguments:
- ancestor_order: int32 [2, 48], replicated, may hold values from 0 to 47, each once within a row
- factor_rows: bfloat16 [2, 24576, 512], P(None, ('row', 'col')), may hold values from -0.0390625 to 0.0390625
- factor_inverse: bfloat16 [2, 512, 512], replicated
- ancestor_inverse: bfloat16 [24576, 24576], P('col', 'row'), may hold values from -6 to 6
- diagonal_inverse: float32 [2, 512, 512], P(None, None, 'row'), may hold values from -6 to 6
Outputs:
- offdiag_inverse: bfloat16 [2, 24576, 512], P(None, 'col', 'row')
- diag_updated: float32 [2, 512, 512], P(None, None, 'row')
The draws below stay inside these ranges and needn't reach their ends.
Inputs may be any that keep to these rules, and one draw needn't show every extreme that they name: `ancestor_order`: each row lists every ancestor block once; its first 40 entries are the blocks coupled to that supernode.
All inputs are finite; a program needn't handle non-finite values.
Results may differ from the reference program's by a relative error of at most 0.011.
Values may be sent and summed in bfloat16 or wider, within the bound.
A program may use at most 128 MiB of HBM per device.

```python
import math
import jax
import jax.numpy as jnp
from jax import lax

B = 512
NA = 48
NSEL = 40
NSUP = 2


def draw_factor_inverse(key, part):
    noise = jax.random.normal(key, (NSUP, B, B), jnp.float32) * (0.6 / math.sqrt(B))
    lower = jnp.tril(noise, -1) + jnp.eye(B, dtype=jnp.float32)[None, :, :]
    return lower.astype(jnp.bfloat16)


def steps_of(key, dims, cuts, low, high):
    loudness = 1.0
    for position, blocks in cuts:
        heights = jax.random.uniform(jax.random.fold_in(jax.random.fold_in(key, 6), position), (blocks,), jnp.float32, low / len(cuts), high / len(cuts))
        loudness = loudness * jnp.repeat(jnp.exp(heights), dims[position] // blocks).reshape((-1,) + (1,) * (len(dims) - 1 - position))
    return loudness


def gaussian(key, dims, width, reach, split=(), kind=jnp.bfloat16):
    entries = width * jax.random.normal(key, dims, jnp.float32)
    if split:
        entries = entries * steps_of(key, dims, split, -0.22, 0.18)
    return jnp.clip(entries, -reach, reach).astype(kind)


def setup_inputs(seed: int = 0) -> dict:
    streams_of = jax.random.split(jax.random.key(seed), 6)
    return {
        "ancestor_order": jax.vmap(lambda own: jax.random.permutation(own, NA))(jax.random.split(streams_of[0], NSUP)).reshape((NSUP, NA)).astype(jnp.int32),
        "factor_rows": gaussian(streams_of[1], (NSUP, NA * B, B), (NA * B) ** -0.5, 0.0390625, ((1, 32),)),
        "factor_inverse": draw_factor_inverse(jax.random.fold_in(streams_of[5], 71), 0),
        "ancestor_inverse": gaussian(streams_of[3], (NA * B, NA * B), 1.0, 6.0, ((0, 8), (1, 4))),
        "diagonal_inverse": gaussian(streams_of[4], (NSUP, B, B), 1.0, 6.0, ((2, 4),), jnp.float32),
    }


def reference(ancestor_order, factor_rows, factor_inverse, ancestor_inverse, diagonal_inverse):
    block_width = factor_rows.shape[2]
    chosen = ancestor_order[:, :NSEL]
    labels = jnp.arange(NA, dtype=jnp.int32)
    block_mask = jnp.any(chosen[:, :, None] == labels[None, None, :], axis=1).astype(jnp.float32)
    row_mask = jnp.repeat(block_mask, block_width, axis=1)
    offdiag_list = []
    diag_list = []
    for index in range(NSUP):
        normed = jnp.dot(factor_rows[index], factor_inverse[index], preferred_element_type=jnp.float32)
        normed = (normed * row_mask[index][:, None]).astype(jnp.bfloat16)
        product = jnp.dot(ancestor_inverse, normed, preferred_element_type=jnp.float32)
        offdiag_list.append((-(product * row_mask[index][:, None])).astype(jnp.bfloat16))
        correction = jnp.dot(normed.astype(jnp.float32).T, product, precision=lax.Precision.HIGHEST)
        diag_list.append(diagonal_inverse[index] + correction)
    return jnp.stack(offdiag_list), jnp.stack(diag_list)
```

```python
import functools

import jax
import jax.numpy as jnp
from jax import lax
from jax.experimental import pallas as pl
from jax.experimental.pallas import tpu as pltpu
from jax.sharding import PartitionSpec as P

NSEL = 40
MESH = pl.DeviceIdType.MESH
TILES = 4
LAG = 4


def kernel(
    dims, strips, order_ref, factor_hbm, inverse_hbm, diag_hbm, a_ref, out_hbm, updated_hbm,
    factor, inverse, diag, outs, updated, panel, abuf, acc, s1, r1, s2, r2, kept, below, cs, cr, total, sums, gsum,
    in_sem, o_sem, a_sem, ring_s, ring_r, s1s, r1s, s2s, r2s, bel_s, bel_r, bel_l, cs_s, cs_r, ag_s, ag_r,
):
    chips, n, depth = dims
    supers, piece, block = factor.shape
    rows, pair = acc.shape[1], acc.shape[2]
    width = pair // 2
    chunks = supers * chips
    half = piece // 2
    tall = rows // TILES
    per_slab = rows // piece
    slabs = n // per_slab
    part = width // n
    r = lax.axis_index("row")
    c = lax.axis_index("col")
    x, k = r // 2, r % 2
    mate = x * 2 + 1 - k
    source_row = c // slabs
    source_x, source_k = source_row // 2, source_row % 2
    source = r == source_row
    passing = (k == source_k) & (x != source_x)
    length = n // depth
    steps = chunks * n

    def col_at(pos):
        y, i = pos // length, pos % length
        return (i + (y % 2) * (length - 1 - 2 * i)) * depth + y

    y, z = c % depth, c // depth
    pos = y * length + z + (y % 2) * (length - 1 - 2 * z)
    right, left = col_at((pos + 1) % n), col_at((pos + n - 1) % n)

    def src_of(j):
        t = (j + 1) // 2
        return col_at((pos + (1 - 2 * (j % 2)) * t + n) % n)

    def a_copy(i):
        src = src_of(i % n)
        if strips:
            view = a_ref.at[src]
        else:
            view = a_ref.at[:, pl.ds(pl.multiple_of(src * piece, piece), piece)]
        return pltpu.make_async_copy(view, abuf.at[i % 2], a_sem.at[i % 2])

    def block_of(g, at_x):
        return (at_x + 1 + g // supers) % chips

    def slot_of(g):
        return (g % supers) * chips + block_of(g, source_x)

    def ring(g, t, d, h, src):
        view = panel.at[g, src, pl.ds(h * half, half)]
        return pltpu.make_async_remote_copy(
            src_ref=view, dst_ref=view,
            send_sem=ring_s.at[d, g, t - 1, h], recv_sem=ring_r.at[d, g, t - 1, h],
            device_id=(r, right * (1 - d) + left * d), device_id_type=MESH,
        )

    def coupled(s, first, count):
        low = order_ref[pl.ds(s, 1), 0:NSEL] * block
        label = first + lax.broadcasted_iota(jnp.int32, (count, NSEL), 0)
        return jnp.sum(jnp.where((label >= low) & (label < low + block), 1.0, 0.0), axis=1, keepdims=True)

    def norm(g, h):
        s = g % supers
        keep = coupled(s, (r * n + c) * piece + h * half, half)
        at = pl.ds(pl.multiple_of(block_of(g, x) * pair, pair), pair)
        term = jnp.dot(factor[s, h * half:(h + 1) * half, :], inverse[s, :, at], preferred_element_type=jnp.float32)
        panel[g, c, h * half:(h + 1) * half, :] = (term * keep).astype(jnp.bfloat16)

    def below_copy(slot, at, src, to_row, sem):
        return pltpu.make_async_remote_copy(
            src_ref=src, dst_ref=below.at[slot, at], send_sem=sem, recv_sem=bel_r.at[slot, at],
            device_id=(to_row, c), device_id_type=MESH,
        )

    def below_here(slot, at, g, src):
        return pltpu.make_async_copy(panel.at[g, src], below.at[slot, at], bel_l.at[slot, at])

    def pass_below(i):
        g, src = i // n, src_of(i % n)
        slot, at = slot_of(g), src % per_slab

        @pl.when(passing & (src // per_slab == c % slabs))
        def _():
            copy = below_copy(slot, at, below.at[slot, at], mate, bel_s.at[slot, at, chips])
            copy.wait_recv()
            copy.start()

    def tile(m):
        return pl.ds(pl.multiple_of(m * tall, tall), tall)

    def mate_copy(g, m):
        return pltpu.make_async_remote_copy(
            src_ref=s1.at[g, tile(m)], dst_ref=r1.at[g, tile(m)],
            send_sem=s1s.at[g, m], recv_sem=r1s.at[g, m],
            device_id=(mate, c), device_id_type=MESH,
        )

    def cross_copy(g, m, slot):
        s = g % supers
        return pltpu.make_async_remote_copy(
            src_ref=s2.at[g, tile(m)], dst_ref=r2.at[s, slot, tile(m)],
            send_sem=s2s.at[g, m], recv_sem=r2s.at[s, slot, m],
            device_id=(block_of(g, x) * 2 + k, c), device_id_type=MESH,
        )

    def give(g, m):
        theirs = jnp.where(k == 0, acc[g % 2, tile(m), width:], acc[g % 2, tile(m), :width])
        s1[g, tile(m), :] = theirs.astype(jnp.bfloat16)
        mate_copy(g, m).start()

    def both(g, m):
        mate_copy(g, m).wait_recv()
        mine = jnp.where(k == 0, acc[g % 2, tile(m), :width], acc[g % 2, tile(m), width:])
        return mine + r1[g, tile(m), :].astype(jnp.float32)

    def send_across(g):
        @pl.loop(0, TILES)
        def _(m):
            s2[g, tile(m), :] = both(g, m).astype(jnp.bfloat16)
            cross_copy(g, m, x).start()

    def out_copy(s):
        return pltpu.make_async_copy(outs.at[s], out_hbm.at[s], o_sem.at[s])

    def finish(g, s):
        @pl.loop(0, TILES)
        def _(m):
            whole = both(g, m)
            for delta in range(1, chips):
                slot = (x + delta) % chips
                cross_copy(s, m, slot).wait_recv()
                whole += r2[s, slot, tile(m), :].astype(jnp.float32)
            outs[s, tile(m), :] = (-(whole * kept[s, tile(m), :])).astype(jnp.bfloat16)

    def scatter(s, delta):
        to = (c + delta) % n
        return pltpu.make_async_remote_copy(
            src_ref=cs.at[s, to], dst_ref=cr.at[s, delta],
            send_sem=cs_s.at[s, delta], recv_sem=cs_r.at[s, delta],
            device_id=(r, to), device_id_type=MESH,
        )

    def gather(s, delta, slot):
        return pltpu.make_async_remote_copy(
            src_ref=total.at[s], dst_ref=sums.at[s, slot],
            send_sem=ag_s.at[s, delta], recv_sem=ag_r.at[s, delta],
            device_id=(r, (c + delta) % n), device_id_type=MESH,
        )

    def correct(s, first, last):
        @pl.loop(first, last)
        def _(j):
            src = src_of(j)
            at = src % per_slab

            @pl.when(src // per_slab == c % slabs)
            def _():
                for e in range(chips):
                    g = e * supers + s
                    slot = slot_of(g)

                    @pl.when(source)
                    def _():
                        below_here(slot, at, g, src).wait()

                    @pl.when(k != source_k)
                    def _():
                        below_copy(slot, at, below.at[slot, at], mate, bel_s.at[slot, at, chips]).wait_recv()

                left = outs[s, pl.ds(pl.multiple_of(at * piece, piece), piece), :]
                for b in range(chips):
                    gsum[:, b * pair:(b + 1) * pair] -= lax.dot_general(
                        left, below[s * chips + b, at], (((0,), (0,)), ((), ())), preferred_element_type=jnp.float32
                    )

    def spread(s):
        for b in range(n):
            cs[s, b] = gsum[b * part:(b + 1) * part, :].astype(jnp.bfloat16)
        for delta in range(1, n):
            scatter(s, delta).start()

    def collect(s):
        summed = cs[s, c].astype(jnp.float32)
        for delta in range(1, n):
            scatter(s, delta).wait_recv()
            summed += cr[s, delta].astype(jnp.float32)
        total[s] = summed.astype(jnp.bfloat16)
        for delta in range(1, n):
            gather(s, delta, c).start()
        sums[s, c] = summed.astype(jnp.bfloat16)

    def updated_copy(s):
        return pltpu.make_async_copy(updated.at[s], updated_hbm.at[s], o_sem.at[supers + s])

    def update(s):
        for delta in range(1, n):
            gather(s, delta, (c + n - delta) % n).wait_recv()
        for b in range(n):
            gsum[b * part:(b + 1) * part, :] = sums[s, b].astype(jnp.float32)
        updated[s] = diag[s] + gsum[...].T
        updated_copy(s).start()

    def factor_copy(s):
        return pltpu.make_async_copy(factor_hbm.at[s], factor.at[s], in_sem.at[s])

    def inverse_copy(s):
        return pltpu.make_async_copy(inverse_hbm.at[s], inverse.at[s], in_sem.at[supers + s])

    diag_copy = pltpu.make_async_copy(diag_hbm, diag, in_sem.at[2 * supers])

    barrier = pltpu.get_barrier_semaphore()
    for delta in range(1, n):
        pl.semaphore_signal(barrier, inc=1, device_id=(r, (c + delta) % n), device_id_type=MESH)
    pl.semaphore_signal(barrier, inc=1, device_id=(mate, c), device_id_type=MESH)
    for delta in range(1, chips):
        pl.semaphore_signal(barrier, inc=1, device_id=(((x + delta) % chips) * 2 + k, c), device_id_type=MESH)
    for s in range(supers):
        factor_copy(s).start()
        inverse_copy(s).start()
    a_copy(0).start()
    diag_copy.start()
    factor_copy(0).wait()
    inverse_copy(0).wait()
    norm(0, 0)
    pl.semaphore_wait(barrier, n - 1 + 1 + chips - 1)
    for h in range(2):
        if h:
            norm(0, h)
        for d in range(2):
            ring(0, 1, d, h, c).start()
    for s in range(1, supers):
        factor_copy(s).wait()
        inverse_copy(s).wait()
    for g in range(1, chunks):
        for h in range(2):
            norm(g, h)
    for s in range(supers):
        @pl.loop(0, TILES)
        def _(m):
            kept[s, tile(m), :] = jnp.broadcast_to(coupled(s, c * rows + m * tall, tall), (tall, width))

    @pl.loop(0, steps)
    def _(i):
        g, j = i // n, i % n
        src = src_of(j)
        ahead, h = j // 2 + 1, j % 2

        @pl.when(ahead < n // 2)
        def _():
            for way in range(2):
                come = col_at((pos + (2 * way - 1) * ahead + n) % n)
                ring(g, ahead, way, h, come).wait_recv()

                @pl.when((ahead + 1 < n // 2) | (h == way))
                def _():
                    ring(g, ahead + 1, way, h, come).start()

        @pl.when((j == n - 3) & (g < chunks - 1))
        def _():
            for first in range(2):
                for way in range(2):
                    ring(g + 1, 1, way, first, c).start()

        @pl.when(j == n - 1)
        def _():
            for way in range(2):
                ring(g, n // 2, way, way, src).wait_recv()

        @pl.when(source & (src // per_slab == c % slabs))
        def _():
            slot, at = slot_of(g), src % per_slab
            for delta in range(1, chips):
                to = ((x + delta) % chips) * 2 + k
                below_copy(slot, at, panel.at[g, src], to, bel_s.at[slot, at, delta]).start()
            below_copy(slot, at, panel.at[g, src], mate, bel_s.at[slot, at, chips]).start()
            below_here(slot, at, g, src).start()

        @pl.when(i >= LAG)
        def _():
            pass_below(i - LAG)

        a_copy(i).wait()

        @pl.when(i + 1 < steps)
        def _():
            a_copy(i + 1).start()

        @pl.loop(0, TILES)
        def _(m):
            term = jnp.dot(abuf[i % 2, tile(m), :], panel[g, src], preferred_element_type=jnp.float32)

            @pl.when(j == 0)
            def _():
                acc[g % 2, tile(m), :] = term

            @pl.when(j > 0)
            def _():
                acc[g % 2, tile(m), :] += term

            @pl.when(j == n - 1)
            def _():
                give(g, m)

        @pl.when((j == 1) & (g > 0) & (g <= chunks - supers))
        def _():
            send_across(g - 1)

        for s in range(supers - 1):
            own = chunks - supers + s

            @pl.when((j == 1) & (g == own + 1))
            def _():
                finish(own, s)
                out_copy(s).start()

            @pl.when((j == n // 2) & (g == own + 1))
            def _():
                gsum[...] = jnp.zeros_like(gsum)
                correct(s, 0, n)
                spread(s)

            @pl.when((j == n - 2) & (g == own + 1))
            def _():
                collect(s)

    last = supers - 1
    for i in range(steps - LAG, steps - 1):
        pass_below(i)
    finish(chunks - 1, last)
    out_copy(last).start()
    for s in range(supers - 1):
        if s == 0:
            diag_copy.wait()
        update(s)
    gsum[...] = jnp.zeros_like(gsum)
    correct(last, 0, n - 1)
    pass_below(steps - 1)
    correct(last, n - 1, n)
    spread(last)
    if supers == 1:
        diag_copy.wait()
    collect(last)
    update(last)
    for s in range(supers):
        for delta in range(1, n):
            scatter(s, delta).wait_send()
            gather(s, delta, c).wait_send()

    @pl.loop(0, chunks)
    def _(g):
        @pl.loop(1, n // 2 + 1)
        def _(t):
            for d in range(2):
                for h in range(2):
                    @pl.when((t < n // 2) | (h == d))
                    def _():
                        ring(g, t, d, h, c).wait_send()

        slot = slot_of(g)
        for at in range(per_slab):
            @pl.when(source)
            def _():
                for delta in range(1, chips):
                    below_copy(slot, at, panel.at[g, c], mate, bel_s.at[slot, at, delta]).wait_send()
                below_copy(slot, at, panel.at[g, c], mate, bel_s.at[slot, at, chips]).wait_send()

            @pl.when(passing)
            def _():
                below_copy(slot, at, below.at[slot, at], mate, bel_s.at[slot, at, chips]).wait_send()

        for m in range(TILES):
            mate_copy(g, m).wait_send()

            @pl.when(g < chunks - supers)
            def _():
                cross_copy(g, m, x).wait_send()

    for s in range(supers):
        out_copy(s).wait()
        updated_copy(s).wait()


def body(ancestor_order, factor_rows, factor_inverse, ancestor_inverse, diagonal_inverse):
    supers, piece, block = factor_rows.shape
    rows = ancestor_inverse.shape[0]
    row_count, n = lax.axis_size("row"), lax.axis_size("col")
    chips = row_count // 2
    depth = chips
    width = block // row_count
    pair = 2 * width
    chunks = supers * chips

    strips = piece % 128 != 0
    left = ancestor_inverse
    if strips:
        left = left.reshape(rows, n, piece).transpose(1, 0, 2)
    per_slab = rows // piece
    part = width // n
    half_type, full_type, dma = jnp.bfloat16, jnp.float32, pltpu.SemaphoreType.DMA
    anywhere = pl.BlockSpec(memory_space=pl.ANY)
    return pl.pallas_call(
        functools.partial(kernel, (chips, n, depth), strips),
        out_shape=(
            jax.ShapeDtypeStruct((supers, rows, width), half_type),
            jax.ShapeDtypeStruct((supers, block, width), full_type),
        ),
        in_specs=[pl.BlockSpec(memory_space=pltpu.VMEM)] + [anywhere] * 4,
        out_specs=(anywhere,) * 2,
        scratch_shapes=[
            pltpu.VMEM((supers, piece, block), half_type),
            pltpu.VMEM((supers, block, block), half_type),
            pltpu.VMEM((supers, block, width), full_type),
            pltpu.VMEM((supers, rows, width), half_type),
            pltpu.VMEM((supers, block, width), full_type),
            pltpu.VMEM((chunks, n, piece, pair), half_type),
            pltpu.VMEM((2, rows, piece), half_type),
            pltpu.VMEM((2, rows, pair), full_type),
            pltpu.VMEM((chunks, rows, width), half_type),
            pltpu.VMEM((chunks, rows, width), half_type),
            pltpu.VMEM((chunks - supers, rows, width), half_type),
            pltpu.VMEM((supers, chips, rows, width), half_type),
            pltpu.VMEM((supers, rows, width), full_type),
            pltpu.VMEM((chunks, per_slab, piece, pair), half_type),
            pltpu.VMEM((supers, n, part, block), half_type),
            pltpu.VMEM((supers, n, part, block), half_type),
            pltpu.VMEM((supers, part, block), half_type),
            pltpu.VMEM((supers, n, part, block), half_type),
            pltpu.VMEM((width, block), full_type),
            dma((2 * supers + 1,)),
            dma((2 * supers,)),
            dma((2,)),
            dma((2, chunks, n // 2, 2)),
            dma((2, chunks, n // 2, 2)),
            dma((chunks, TILES)),
            dma((chunks, TILES)),
            dma((chunks - supers, TILES)),
            dma((supers, chips, TILES)),
            dma((chunks, per_slab, chips + 1)),
            dma((chunks, per_slab)),
            dma((chunks, per_slab)),
            dma((supers, n)),
            dma((supers, n)),
            dma((supers, n)),
            dma((supers, n)),
        ],
        compiler_params=pltpu.CompilerParams(
            collective_id=0, has_side_effects=True, vmem_limit_bytes=64 * 1024 * 1024 - 65536
        ),
        cost_estimate=pl.CostEstimate(
            flops=2 * rows * n * piece * supers * block, bytes_accessed=8 * rows * n * piece, transcendentals=0
        ),
    )(ancestor_order, factor_rows, factor_inverse, diagonal_inverse, left)


def solution(mesh):
    placed = (P(), P(None, ("row", "col"), None), P(), P("col", "row"), P(None, None, "row"))
    return jax.shard_map(
        body,
        mesh=mesh,
        in_specs=placed,
        out_specs=(P(None, "col", "row"), P(None, None, "row")),
        check_vma=False,
    )
```

```python
import functools

import jax
import jax.numpy as jnp
from jax import lax
from jax.experimental import pallas as pl
from jax.experimental.pallas import tpu as pltpu
from jax.sharding import PartitionSpec as P

NSEL = 40
MESH = pl.DeviceIdType.MESH
TILES = 2
LAG = 6
NEAR = 2
BEGIN = 2
DEEP = 3


def kernel(
    dims, strips, order_ref, factor_hbm, inverse_hbm, diag_hbm, a_ref, out_hbm, updated_hbm,
    factor, inverse, diag, outs, updated, panel, abuf, acc, s1, r1, s2, r2, kept, moved, below, cs, cr, total, sums, gsum,
    in_sem, o_sem, a_sem, ring_s, ring_r, s1s, r1s, s2s, r2s, mov_s, mov_r, bel_s, bel_r, bel_l, cs_s, cs_r, ag_s, ag_r,
):
    chips, n, depth = dims
    supers, piece, block = factor.shape
    rows, pair = acc.shape[1], acc.shape[2]
    width = pair // 2
    chunks = supers * chips
    half = piece // 2
    tall = rows // TILES
    per_slab = rows // piece
    slabs = n // per_slab
    part = width // n
    r = lax.axis_index("row")
    c = lax.axis_index("col")
    x, k = r // 2, r % 2
    mate = x * 2 + 1 - k
    source_row = c // slabs
    source_x, source_k = source_row // 2, source_row % 2
    source = r == source_row
    passing = (k == source_k) & (x != source_x)
    home = x == source_x
    last = supers - 1
    length = n // depth
    steps = chunks * n

    def col_at(pos):
        y, i = pos // length, pos % length
        return (i + (y % 2) * (length - 1 - 2 * i)) * depth + y

    y, z = c % depth, c // depth
    pos = y * length + z + (y % 2) * (length - 1 - 2 * z)
    right, left = col_at((pos + 1) % n), col_at((pos + n - 1) % n)

    def src_of(j):
        t = (j + 1) // 2
        return col_at((pos + (1 - 2 * (j % 2)) * t + n) % n)

    def a_copy(i):
        src = src_of(i % n)
        if strips:
            view = a_ref.at[src]
        else:
            view = a_ref.at[:, pl.ds(pl.multiple_of(src * piece, piece), piece)]
        return pltpu.make_async_copy(view, abuf.at[i % DEEP], a_sem.at[i % DEEP])

    def block_of(g, at_x):
        return (at_x + 1 + g // supers) % chips

    def slot_of(g):
        return (g % supers) * chips + block_of(g, source_x)

    def ring(g, t, d, q, src):
        h = q + d - 2 * q * d
        view = panel.at[g, src, pl.ds(h * half, half)]
        return pltpu.make_async_remote_copy(
            src_ref=view, dst_ref=view,
            send_sem=ring_s.at[g], recv_sem=ring_r.at[d, g % 2, t - 1, q],
            device_id=(r, right * (1 - d) + left * d), device_id_type=MESH,
        )

    def coupled(s, first, count):
        low = order_ref[pl.ds(s, 1), 0:NSEL] * block
        label = first + lax.broadcasted_iota(jnp.int32, (count, NSEL), 0)
        return jnp.sum(jnp.where((label >= low) & (label < low + block), 1.0, 0.0), axis=1, keepdims=True)

    def norm(g, h):
        s = g % supers
        keep = coupled(s, (r * n + c) * piece + h * half, half)
        at = pl.ds(pl.multiple_of(block_of(g, x) * pair, pair), pair)
        term = jnp.dot(factor[s, h * half:(h + 1) * half, :], inverse[s, :, at], preferred_element_type=jnp.float32)
        panel[g, c, h * half:(h + 1) * half, :] = (term * keep).astype(jnp.bfloat16)

    def below_copy(slot, at, src, to_row, sem):
        return pltpu.make_async_remote_copy(
            src_ref=src, dst_ref=below.at[slot, at], send_sem=sem, recv_sem=bel_r.at[slot, at],
            device_id=(to_row, c), device_id_type=MESH,
        )

    def below_here(slot, at, g, src):
        return pltpu.make_async_copy(panel.at[g, src], below.at[slot, at], bel_l.at[slot])

    def lend(g, j):
        src = src_of(j)
        slot, at = slot_of(g), src % per_slab

        @pl.when(source & (src // per_slab == c % slabs))
        def _():
            below_copy(slot, at, panel.at[g, src], mate, bel_s.at[0]).start()
            below_here(slot, at, g, src).start()

    def lend_half(g, src, h):
        slot, at = slot_of(g), src % per_slab
        view = pl.ds(pl.multiple_of(h * half, half), half)

        @pl.when(source & (g % supers == last) & (src // per_slab == c % slabs))
        def _():
            for delta in range(1, chips):
                pltpu.make_async_remote_copy(
                    src_ref=panel.at[g, src, view], dst_ref=below.at[slot, at, view],
                    send_sem=bel_s.at[delta], recv_sem=bel_r.at[slot, at],
                    device_id=(((x + delta) % chips) * 2 + k, c), device_id_type=MESH,
                ).start()

    def pass_below(i):
        g, src = i // n, src_of(i % n)
        slot, at = slot_of(g), src % per_slab

        @pl.when(passing & (g % supers == last) & (src // per_slab == c % slabs))
        def _():
            copy = below_copy(slot, at, below.at[slot, at], mate, bel_s.at[0])
            copy.wait_recv()
            copy.start()

    def tile(m):
        return pl.ds(pl.multiple_of(m * tall, tall), tall)

    def mate_copy(g, m):
        return pltpu.make_async_remote_copy(
            src_ref=s1.at[g, tile(m)], dst_ref=r1.at[g, tile(m)],
            send_sem=s1s.at[0], recv_sem=r1s.at[g, m],
            device_id=(mate, c), device_id_type=MESH,
        )

    def cross_copy(g, m, slot):
        s = g % supers
        return pltpu.make_async_remote_copy(
            src_ref=s2.at[g, tile(m)], dst_ref=r2.at[s, slot, tile(m)],
            send_sem=s2s.at[0], recv_sem=r2s.at[s, slot],
            device_id=(block_of(g, x) * 2 + k, c), device_id_type=MESH,
        )

    def give(g, m):
        theirs = jnp.where(k == 0, acc[g % 2, tile(m), width:], acc[g % 2, tile(m), :width])
        s1[g, tile(m), :] = theirs.astype(jnp.bfloat16)
        mate_copy(g, m).start()

    def both(g, m):
        mate_copy(g, m).wait_recv()
        mine = jnp.where(k == 0, acc[g % 2, tile(m), :width], acc[g % 2, tile(m), width:])
        return mine + r1[g, tile(m), :].astype(jnp.float32)

    def send_across(g, m):
        s2[g, tile(m), :] = both(g, m).astype(jnp.bfloat16)
        cross_copy(g, m, x).start()

    def out_copy(s):
        return pltpu.make_async_copy(outs.at[s], out_hbm.at[s], o_sem.at[s])

    def cross_wait(s, slot):
        pltpu.make_async_remote_copy(
            src_ref=s2.at[0], dst_ref=r2.at[s, slot], send_sem=s2s.at[0], recv_sem=r2s.at[s, slot],
            device_id=(mate, c), device_id_type=MESH,
        ).wait_recv()

    def finish(g, s):
        for delta in range(1, chips):
            cross_wait(s, (x + delta) % chips)

        @pl.loop(0, TILES)
        def _(m):
            whole = both(g, m)
            for delta in range(1, chips):
                whole += r2[s, (x + delta) % chips, tile(m), :].astype(jnp.float32)
            outs[s, tile(m), :] = (-(whole * kept[s, tile(m), :])).astype(jnp.bfloat16)

    def move(s, slot):
        return pltpu.make_async_remote_copy(
            src_ref=outs.at[s], dst_ref=moved.at[s, slot], send_sem=mov_s.at[s], recv_sem=mov_r.at[s, slot],
            device_id=(source_x * 2 + k, c), device_id_type=MESH,
        )

    def piece_copy(s, first, count, slot, plane, to):
        return pltpu.make_async_remote_copy(
            src_ref=cs.at[s, pl.ds(first, count)], dst_ref=cr.at[s, pl.ds(slot, count)],
            send_sem=cs_s.at[s], recv_sem=cs_r.at[s],
            device_id=(plane * 2 + k, to), device_id_type=MESH,
        )

    def gather(s, slot, count, to):
        return pltpu.make_async_remote_copy(
            src_ref=total.at[s, pl.ds(0, count)], dst_ref=sums.at[s, pl.ds(slot, count)],
            send_sem=ag_s.at[s], recv_sem=ag_r.at[s],
            device_id=(r, to), device_id_type=MESH,
        )

    def below_wait(s):
        for e in range(chips):
            slot = slot_of(e * supers + s)

            @pl.when(source)
            def _():
                pltpu.make_async_copy(below.at[slot], below.at[slot], bel_l.at[slot]).wait()

    def correct(s, first, end, left_of):
        @pl.loop(first, end)
        def _(j):
            src = src_of(j)
            at = src % per_slab

            @pl.when(src // per_slab == c % slabs)
            def _():
                left = left_of(pl.ds(pl.multiple_of(at * piece, piece), piece))
                for b in range(chips):
                    gsum[:, b * pair:(b + 1) * pair] -= lax.dot_general(
                        left, below[s * chips + b, at], (((0,), (0,)), ((), ())), preferred_element_type=jnp.float32
                    )

    def below_arrived(s, first, end):
        @pl.loop(first, end)
        def _(j):
            src = src_of(j)
            at = src % per_slab

            @pl.when((k != source_k) & (src // per_slab == c % slabs))
            def _():
                for e in range(chips):
                    slot = slot_of(e * supers + s)
                    below_copy(slot, at, below.at[slot, at], mate, bel_s.at[0]).wait_recv()

    def fill(s, delta):
        for b in range(n):
            cs[s, delta * n + b] = gsum[b * part:(b + 1) * part, :].astype(jnp.bfloat16)
        if delta == 0:
            cr[s, c] = cs[s, c]

    def spread(s, delta):
        plane = (x + delta) % chips
        for ahead in range(0 if delta else 1, n):
            to = (c + ahead) % n
            piece_copy(s, delta * n + to, 1, c, plane, to).start()

    def early_own(s):
        @pl.when(home)
        def _():
            below_wait(s)
            below_arrived(s, 0, n)
            gsum[...] = jnp.zeros_like(gsum)
            correct(s, 0, n, lambda at: outs[s, at, :])
            fill(s, 0)

    def early_other(s):
        for delta in range(1, chips):
            plane = (x + delta) % chips
            move(s, plane).wait_recv()
            gsum[...] = jnp.zeros_like(gsum)
            correct(s, 0, n, lambda at: moved[s, plane, at, :])
            fill(s, delta)

    def early_send(s):
        @pl.when(home)
        def _():
            for delta in range(1, chips):
                spread(s, delta)

    def collect(s):
        if s == last:
            piece_copy(s, 0, n - 1, 0, x, c).wait_recv()
        else:
            @pl.when(home)
            def _():
                piece_copy(s, 0, n - 1, 0, x, c).wait_recv()

            @pl.when(x != source_x)
            def _():
                piece_copy(s, 0, n, 0, x, c).wait_recv()
        summed = cr[s, 0].astype(jnp.float32)
        for b in range(1, n):
            summed += cr[s, b].astype(jnp.float32)
        total[s, 0] = summed.astype(jnp.bfloat16)
        for ahead in range(1, n):
            gather(s, c, 1, (c + ahead) % n).start()
        sums[s, c] = summed.astype(jnp.bfloat16)

    def updated_copy(s):
        return pltpu.make_async_copy(updated.at[s], updated_hbm.at[s], o_sem.at[supers + s])

    def update(s):
        pltpu.make_async_remote_copy(
            src_ref=sums.at[s, pl.ds(0, n - 1)], dst_ref=sums.at[s, pl.ds(0, n - 1)],
            send_sem=ag_s.at[s], recv_sem=ag_r.at[s], device_id=(mate, c), device_id_type=MESH,
        ).wait_recv()
        for b in range(n):
            gsum[b * part:(b + 1) * part, :] = sums[s, b].astype(jnp.float32)
        updated[s] = diag[s] + gsum[...].T
        updated_copy(s).start()

    def factor_copy(s):
        return pltpu.make_async_copy(factor_hbm.at[s], factor.at[s], in_sem.at[s])

    def inverse_copy(s):
        return pltpu.make_async_copy(inverse_hbm.at[s], inverse.at[s], in_sem.at[supers + s])

    def sent(ref, sem):
        pltpu.make_async_remote_copy(
            src_ref=ref, dst_ref=ref, send_sem=sem, recv_sem=sem, device_id=(mate, c), device_id_type=MESH
        ).wait_send()

    def drain():
        for g in range(chunks):
            sent(panel.at[g, pl.ds(0, n - 1)], ring_s.at[g])
        sent(s1, s1s.at[0])
        sent(s2, s2s.at[0])
        ending = below.at[pl.ds(last * chips, chips)]

        @pl.when(source)
        def _():
            sent(below, bel_s.at[0])
            for delta in range(1, chips):
                sent(ending, bel_s.at[delta])

        @pl.when(passing)
        def _():
            sent(ending, bel_s.at[0])

        for s in range(last):
            @pl.when(x != source_x)
            def _():
                sent(outs.at[s], mov_s.at[s])

    def pieces_sent(s):
        if s == last:
            sent(cs.at[s, pl.ds(0, n - 1)], cs_s.at[s])
        else:
            @pl.when(home)
            def _():
                sent(cs.at[s, pl.ds(0, chips * n - 1)], cs_s.at[s])
        sent(sums.at[s, pl.ds(0, n - 1)], ag_s.at[s])

    diag_copy = pltpu.make_async_copy(diag_hbm, diag, in_sem.at[2 * supers])

    barrier = pltpu.get_barrier_semaphore()
    pl.semaphore_signal(barrier, inc=1, device_id=(mate, c), device_id_type=MESH)
    for delta in range(chips):
        for ahead in range(0 if delta else 1, n):
            there = (((x + delta) % chips) * 2 + k, (c + ahead) % n)
            pl.semaphore_signal(barrier, inc=1, device_id=there, device_id_type=MESH)
    for s in range(supers):
        factor_copy(s).start()
        inverse_copy(s).start()
    for i in range(DEEP - 1):
        a_copy(i).start()
    diag_copy.start()
    factor_copy(0).wait()
    inverse_copy(0).wait()
    norm(0, 0)
    pl.semaphore_wait(barrier, chips * n)
    ring(0, 1, 0, 0, c).start()
    norm(0, 1)
    ring(0, 1, 1, 0, c).start()
    for d in range(2):
        ring(0, 1, d, 1, c).start()
    for s in range(1, supers):
        factor_copy(s).wait()
        inverse_copy(s).wait()
    for g in range(1, chunks):
        for h in range(2):
            norm(g, h)
    for s in range(supers):
        @pl.loop(0, TILES)
        def _(m):
            kept[s, tile(m), :] = jnp.broadcast_to(coupled(s, c * rows + m * tall, tall), (tall, width))

    @pl.loop(0, steps)
    def _(i):
        g, j = i // n, i % n
        src = src_of(j)
        ahead, q = j // 2 + 1, j % 2

        @pl.when(ahead < n // 2)
        def _():
            for way in range(2):
                come = col_at((pos + (2 * way - 1) * ahead + n) % n)
                ring(g, ahead, way, q, come).wait_recv()

                @pl.when((ahead + 1 < n // 2) | (q == 0))
                def _():
                    ring(g, ahead + 1, way, q, come).start()

            for way in range(2):
                come = col_at((pos + (2 * way - 1) * ahead + n) % n)
                lend_half(g, come, q + way - 2 * q * way)

        @pl.when(((j == n - 4) | (j == n - 3)) & (g < chunks - 1))
        def _():
            for way in range(2):
                ring(g + 1, 1, way, q, c).start()

        @pl.when(j == n - 1)
        def _():
            for way in range(2):
                ring(g, n // 2, way, 0, src).wait_recv()
                lend_half(g, src, way)

        @pl.when(j == 0)
        def _():
            for h in range(2):
                lend_half(g, c, h)

        @pl.when((j == 0) | (j % 2 == 1))
        def _():
            lend(g, j)

        @pl.when((j < n - 1) & (j % 2 == 1))
        def _():
            lend(g, j + 1)

        @pl.when((i == steps - 1) & home)
        def _():
            for s in range(last):
                spread(s, 0)
                early_other(s)

        @pl.when((i >= LAG) & (i < steps - 2))
        def _():
            pass_below(i - LAG)

        @pl.when(i == steps - 2)
        def _():
            @pl.loop(steps - 2 - LAG, steps - 1 - NEAR)
            def _(late):
                pass_below(late)

        @pl.when(i == steps - 1)
        def _():
            pass_below(i - NEAR)

        a_copy(i).wait()

        @pl.when(i + DEEP - 1 < steps)
        def _():
            a_copy(i + DEEP - 1).start()

        @pl.loop(0, TILES)
        def _(m):
            term = jnp.dot(abuf[i % DEEP, tile(m), :], panel[g, src], preferred_element_type=jnp.float32)

            @pl.when(j == 0)
            def _():
                acc[g % 2, tile(m), :] = term

            @pl.when(j > 0)
            def _():
                acc[g % 2, tile(m), :] += term

            @pl.when(j == n - 1)
            def _():
                give(g, m)

        @pl.when((j >= BEGIN) & (j < BEGIN + TILES) & (g > 0) & (g <= chunks - supers))
        def _():
            send_across(g - 1, j - BEGIN)

        for s in range(last):
            own = chunks - supers + s

            @pl.when((j == 0) & (g == own + 1))
            def _():
                finish(own, s)
                out_copy(s).start()

                @pl.when(x != source_x)
                def _():
                    move(s, x).start()

            @pl.when((j == 3) & (g == own + 1))
            def _():
                early_own(s)
    for i in range(steps - NEAR, steps - 1):
        pass_below(i)
    finish(chunks - 1, last)
    out_copy(last).start()
    for s in range(last):
        early_send(s)
    gsum[...] = jnp.zeros_like(gsum)
    below_wait(last)
    below_arrived(last, 0, n - 1)
    correct(last, 0, n - 1, lambda at: outs[last, at, :])
    pass_below(steps - 1)
    below_arrived(last, n - 1, n)
    correct(last, n - 1, n, lambda at: outs[last, at, :])
    fill(last, 0)
    spread(last, 0)
    for s in range(last):
        collect(s)
    drain()
    diag_copy.wait()
    collect(last)
    for s in range(supers):
        update(s)
    for s in range(supers):
        pieces_sent(s)
    for s in range(supers):
        out_copy(s).wait()
        updated_copy(s).wait()


def body(ancestor_order, factor_rows, factor_inverse, ancestor_inverse, diagonal_inverse):
    supers, piece, block = factor_rows.shape
    rows = ancestor_inverse.shape[0]
    row_count, n = lax.axis_size("row"), lax.axis_size("col")
    chips = row_count // 2
    depth = chips
    width = block // row_count
    pair = 2 * width
    chunks = supers * chips

    strips = piece % 128 != 0
    left = ancestor_inverse
    if strips:
        left = left.reshape(rows, n, piece).transpose(1, 0, 2)
    per_slab = rows // piece
    part = width // n
    half_type, full_type, dma = jnp.bfloat16, jnp.float32, pltpu.SemaphoreType.DMA
    anywhere = pl.BlockSpec(memory_space=pl.ANY)
    return pl.pallas_call(
        functools.partial(kernel, (chips, n, depth), strips),
        out_shape=(
            jax.ShapeDtypeStruct((supers, rows, width), half_type),
            jax.ShapeDtypeStruct((supers, block, width), full_type),
        ),
        in_specs=[pl.BlockSpec(memory_space=pltpu.VMEM)] + [anywhere] * 4,
        out_specs=(anywhere,) * 2,
        scratch_shapes=[
            pltpu.VMEM((supers, piece, block), half_type),
            pltpu.VMEM((supers, block, block), half_type),
            pltpu.VMEM((supers, block, width), full_type),
            pltpu.VMEM((supers, rows, width), half_type),
            pltpu.VMEM((supers, block, width), full_type),
            pltpu.VMEM((chunks, n, piece, pair), half_type),
            pltpu.VMEM((DEEP, rows, piece), half_type),
            pltpu.VMEM((2, rows, pair), full_type),
            pltpu.VMEM((chunks, rows, width), half_type),
            pltpu.VMEM((chunks, rows, width), half_type),
            pltpu.VMEM((chunks - supers, rows, width), half_type),
            pltpu.VMEM((supers, chips, rows, width), half_type),
            pltpu.VMEM((supers, rows, width), full_type),
            pltpu.VMEM((max(supers - 1, 1), chips, rows, width), half_type),
            pltpu.VMEM((chunks, per_slab, piece, pair), half_type),
            pltpu.VMEM((supers, chips * n, part, block), half_type),
            pltpu.VMEM((supers, n, part, block), half_type),
            pltpu.VMEM((supers, 1, part, block), half_type),
            pltpu.VMEM((supers, n, part, block), half_type),
            pltpu.VMEM((width, block), full_type),
            dma((2 * supers + 1,)),
            dma((2 * supers,)),
            dma((DEEP,)),
            dma((chunks,)),
            dma((2, 2, n // 2, 2)),
            dma((1,)),
            dma((chunks, TILES)),
            dma((1,)),
            dma((supers, chips)),
            dma((max(supers - 1, 1),)),
            dma((max(supers - 1, 1), chips)),
            dma((chips,)),
            dma((chunks, per_slab)),
            dma((chunks,)),
            dma((supers,)),
            dma((supers,)),
            dma((supers,)),
            dma((supers,)),
        ],
        compiler_params=pltpu.CompilerParams(
            collective_id=0, has_side_effects=True, vmem_limit_bytes=64 * 1024 * 1024 - 65536
        ),
        cost_estimate=pl.CostEstimate(
            flops=2 * rows * n * piece * supers * block, bytes_accessed=8 * rows * n * piece, transcendentals=0
        ),
    )(ancestor_order, factor_rows, factor_inverse, diagonal_inverse, left)


def solution(mesh):
    placed = (P(), P(None, ("row", "col"), None), P(), P("col", "row"), P(None, None, "row"))
    return jax.shard_map(
        body,
        mesh=mesh,
        in_specs=placed,
        out_specs=(P(None, "col", "row"), P(None, None, "row")),
        check_vma=False,
    )
```

```python
import functools

import jax
import jax.numpy as jnp
from jax import lax
from jax.experimental import pallas as pl
from jax.experimental.pallas import tpu as pltpu
from jax.sharding import PartitionSpec as P

NSEL = 40
MESH = pl.DeviceIdType.MESH
TILES = 2
LAG = 6
NEAR = 2
BEGIN = 2
DEEP = 3


def kernel(
    dims, strips, order_ref, factor_hbm, inverse_hbm, diag_hbm, a_ref, outs, updated,
    factor, inverse, diag, panel, abuf, acc, s1, r1, s2, r2, kept, moved, below, cs, cr, total, sums, gsum,
    in_sem, a_sem, ring_s, ring_r, s1s, r1s, s2s, r2s, mov_s, mov_r, bel_s, bel_r, bel_l, cs_s, cs_r, ag_s, ag_r,
):
    chips, n, depth = dims
    supers, piece, block = factor.shape
    rows, pair = acc.shape[1], acc.shape[2]
    width = pair // 2
    chunks = supers * chips
    half = piece // 2
    tall = rows // TILES
    per_slab = rows // piece
    slabs = n // per_slab
    part = width // n
    r = lax.axis_index("row")
    c = lax.axis_index("col")
    x, k = r // 2, r % 2
    mate = x * 2 + 1 - k
    source_row = c // slabs
    source_x, source_k = source_row // 2, source_row % 2
    source = r == source_row
    passing = (k == source_k) & (x != source_x)
    home = x == source_x
    last = supers - 1
    length = n // depth
    steps = chunks * n

    def col_at(pos):
        y, i = pos // length, pos % length
        return (i + (y % 2) * (length - 1 - 2 * i)) * depth + y

    y, z = c % depth, c // depth
    pos = y * length + z + (y % 2) * (length - 1 - 2 * z)
    right, left = col_at((pos + 1) % n), col_at((pos + n - 1) % n)

    def src_of(j):
        t = (j + 1) // 2
        return col_at((pos + (1 - 2 * (j % 2)) * t + n) % n)

    def a_copy(i):
        src = src_of(i % n)
        if strips:
            view = a_ref.at[src]
        else:
            view = a_ref.at[:, pl.ds(pl.multiple_of(src * piece, piece), piece)]
        return pltpu.make_async_copy(view, abuf.at[i % DEEP], a_sem.at[i % DEEP])

    def block_of(g, at_x):
        return (at_x + 1 + g // supers) % chips

    def slot_of(g):
        return (g % supers) * chips + block_of(g, source_x)

    def ring(g, t, d, q, src):
        h = q + d - 2 * q * d
        view = panel.at[g, src, pl.ds(h * half, half)]
        return pltpu.make_async_remote_copy(
            src_ref=view, dst_ref=view,
            send_sem=ring_s.at[g], recv_sem=ring_r.at[d, g % 2, t - 1, q],
            device_id=(r, right * (1 - d) + left * d), device_id_type=MESH,
        )

    def coupled(s, first, count):
        low = order_ref[pl.ds(s, 1), 0:NSEL] * block
        label = first + lax.broadcasted_iota(jnp.int32, (count, NSEL), 0)
        return jnp.sum(jnp.where((label >= low) & (label < low + block), 1.0, 0.0), axis=1, keepdims=True)

    def norm(g, h):
        s = g % supers
        keep = coupled(s, (r * n + c) * piece + h * half, half)
        at = pl.ds(pl.multiple_of(block_of(g, x) * pair, pair), pair)
        term = jnp.dot(factor[s, h * half:(h + 1) * half, :], inverse[s, :, at], preferred_element_type=jnp.float32)
        panel[g, c, h * half:(h + 1) * half, :] = (term * keep).astype(jnp.bfloat16)

    def below_copy(slot, at, src, to_row, sem):
        return pltpu.make_async_remote_copy(
            src_ref=src, dst_ref=below.at[slot, at], send_sem=sem, recv_sem=bel_r.at[slot, at],
            device_id=(to_row, c), device_id_type=MESH,
        )

    def below_here(slot, at, g, src):
        return pltpu.make_async_copy(panel.at[g, src], below.at[slot, at], bel_l.at[slot])

    def lend(g, j):
        src = src_of(j)
        slot, at = slot_of(g), src % per_slab

        @pl.when(source & (src // per_slab == c % slabs))
        def _():
            below_copy(slot, at, panel.at[g, src], mate, bel_s.at[0]).start()
            below_here(slot, at, g, src).start()

    def lend_half(g, src, h):
        slot, at = slot_of(g), src % per_slab
        view = pl.ds(pl.multiple_of(h * half, half), half)

        @pl.when(source & (g % supers == last) & (src // per_slab == c % slabs))
        def _():
            for delta in range(1, chips):
                pltpu.make_async_remote_copy(
                    src_ref=panel.at[g, src, view], dst_ref=below.at[slot, at, view],
                    send_sem=bel_s.at[delta], recv_sem=bel_r.at[slot, at],
                    device_id=(((x + delta) % chips) * 2 + k, c), device_id_type=MESH,
                ).start()

    def pass_below(i):
        g, src = i // n, src_of(i % n)
        slot, at = slot_of(g), src % per_slab

        @pl.when(passing & (g % supers == last) & (src // per_slab == c % slabs))
        def _():
            copy = below_copy(slot, at, below.at[slot, at], mate, bel_s.at[0])
            copy.wait_recv()
            copy.start()

    def tile(m):
        return pl.ds(pl.multiple_of(m * tall, tall), tall)

    def mate_copy(g, m):
        return pltpu.make_async_remote_copy(
            src_ref=s1.at[g, tile(m)], dst_ref=r1.at[g, tile(m)],
            send_sem=s1s.at[0], recv_sem=r1s.at[g, m],
            device_id=(mate, c), device_id_type=MESH,
        )

    def cross_copy(g, m, slot):
        s = g % supers
        return pltpu.make_async_remote_copy(
            src_ref=s2.at[g, tile(m)], dst_ref=r2.at[s, slot, tile(m)],
            send_sem=s2s.at[0], recv_sem=r2s.at[s, slot],
            device_id=(block_of(g, x) * 2 + k, c), device_id_type=MESH,
        )

    def give(g, m):
        theirs = jnp.where(k == 0, acc[g % 2, tile(m), width:], acc[g % 2, tile(m), :width])
        s1[g, tile(m), :] = theirs.astype(jnp.bfloat16)
        mate_copy(g, m).start()

    def both(g, m):
        mate_copy(g, m).wait_recv()
        mine = jnp.where(k == 0, acc[g % 2, tile(m), :width], acc[g % 2, tile(m), width:])
        return mine + r1[g, tile(m), :].astype(jnp.float32)

    def send_across(g, m):
        s2[g, tile(m), :] = both(g, m).astype(jnp.bfloat16)
        cross_copy(g, m, x).start()

    def cross_wait(s, slot):
        pltpu.make_async_remote_copy(
            src_ref=s2.at[0], dst_ref=r2.at[s, slot], send_sem=s2s.at[0], recv_sem=r2s.at[s, slot],
            device_id=(mate, c), device_id_type=MESH,
        ).wait_recv()

    def finish(g, s):
        for delta in range(1, chips):
            cross_wait(s, (x + delta) % chips)

        @pl.loop(0, TILES)
        def _(m):
            whole = both(g, m)
            for delta in range(1, chips):
                whole += r2[s, (x + delta) % chips, tile(m), :].astype(jnp.float32)
            outs[s, tile(m), :] = (-(whole * kept[s, tile(m), :])).astype(jnp.bfloat16)

    def move(s, slot):
        return pltpu.make_async_remote_copy(
            src_ref=outs.at[s], dst_ref=moved.at[s, slot], send_sem=mov_s.at[s], recv_sem=mov_r.at[s, slot],
            device_id=(source_x * 2 + k, c), device_id_type=MESH,
        )

    def piece_copy(s, first, count, slot, plane, to):
        return pltpu.make_async_remote_copy(
            src_ref=cs.at[s, pl.ds(first, count)], dst_ref=cr.at[s, pl.ds(slot, count)],
            send_sem=cs_s.at[s], recv_sem=cs_r.at[s],
            device_id=(plane * 2 + k, to), device_id_type=MESH,
        )

    def gather(s, slot, count, to):
        return pltpu.make_async_remote_copy(
            src_ref=total.at[s, pl.ds(0, count)], dst_ref=sums.at[s, pl.ds(slot, count)],
            send_sem=ag_s.at[s], recv_sem=ag_r.at[s],
            device_id=(r, to), device_id_type=MESH,
        )

    def below_wait(s):
        for e in range(chips):
            slot = slot_of(e * supers + s)

            @pl.when(source)
            def _():
                pltpu.make_async_copy(below.at[slot], below.at[slot], bel_l.at[slot]).wait()

    def correct(s, first, end, left_of):
        @pl.loop(first, end)
        def _(j):
            src = src_of(j)
            at = src % per_slab

            @pl.when(src // per_slab == c % slabs)
            def _():
                left = left_of(pl.ds(pl.multiple_of(at * piece, piece), piece))
                for b in range(chips):
                    gsum[:, b * pair:(b + 1) * pair] -= lax.dot_general(
                        left, below[s * chips + b, at], (((0,), (0,)), ((), ())), preferred_element_type=jnp.float32
                    )

    def below_arrived(s, first, end):
        @pl.loop(first, end)
        def _(j):
            src = src_of(j)
            at = src % per_slab

            @pl.when((k != source_k) & (src // per_slab == c % slabs))
            def _():
                for e in range(chips):
                    slot = slot_of(e * supers + s)
                    below_copy(slot, at, below.at[slot, at], mate, bel_s.at[0]).wait_recv()

    def farthest_first(send):
        for i in range(length):
            there = jnp.where(2 * z < length, length - 1 - i, i)
            for u in range(depth):
                to = there * depth + (y + 1 + u) % depth

                @pl.when(to != c)
                def _():
                    send(to)

    def fill(s, delta):
        for b in range(n):
            cs[s, delta * n + b] = gsum[b * part:(b + 1) * part, :].astype(jnp.bfloat16)
        if delta == 0:
            cr[s, c] = cs[s, c]

    def spread(s, delta):
        plane = (x + delta) % chips

        def send(to):
            piece_copy(s, delta * n + to, 1, c, plane, to).start()

        if delta:
            send(c)
        farthest_first(send)

    def early_own(s):
        @pl.when(home)
        def _():
            below_wait(s)
            below_arrived(s, 0, n)
            gsum[...] = jnp.zeros_like(gsum)
            correct(s, 0, n, lambda at: outs[s, at, :])
            fill(s, 0)

    def early_other(s):
        for delta in range(1, chips):
            plane = (x + delta) % chips
            move(s, plane).wait_recv()
            gsum[...] = jnp.zeros_like(gsum)
            correct(s, 0, n, lambda at: moved[s, plane, at, :])
            fill(s, delta)

    def early_send(s):
        @pl.when(home)
        def _():
            for delta in range(1, chips):
                spread(s, delta)

    def collect(s):
        if s == last:
            piece_copy(s, 0, n - 1, 0, x, c).wait_recv()
        else:
            @pl.when(home)
            def _():
                piece_copy(s, 0, n - 1, 0, x, c).wait_recv()

            @pl.when(x != source_x)
            def _():
                piece_copy(s, 0, n, 0, x, c).wait_recv()
        summed = cr[s, 0].astype(jnp.float32)
        for b in range(1, n):
            summed += cr[s, b].astype(jnp.float32)
        total[s, 0] = summed.astype(jnp.bfloat16)
        farthest_first(lambda to: gather(s, c, 1, to).start())
        sums[s, c] = summed.astype(jnp.bfloat16)

    def update(s):
        pltpu.make_async_remote_copy(
            src_ref=sums.at[s, pl.ds(0, n - 1)], dst_ref=sums.at[s, pl.ds(0, n - 1)],
            send_sem=ag_s.at[s], recv_sem=ag_r.at[s], device_id=(mate, c), device_id_type=MESH,
        ).wait_recv()
        for b in range(n):
            gsum[b * part:(b + 1) * part, :] = sums[s, b].astype(jnp.float32)
        updated[s] = diag[s] + gsum[...].T

    def factor_copy(s):
        return pltpu.make_async_copy(factor_hbm.at[s], factor.at[s], in_sem.at[s])

    def inverse_copy(s):
        return pltpu.make_async_copy(inverse_hbm.at[s], inverse.at[s], in_sem.at[supers + s])

    def sent(ref, sem):
        pltpu.make_async_remote_copy(
            src_ref=ref, dst_ref=ref, send_sem=sem, recv_sem=sem, device_id=(mate, c), device_id_type=MESH
        ).wait_send()

    def drain():
        for g in range(chunks):
            sent(panel.at[g, pl.ds(0, n - 1)], ring_s.at[g])
        sent(s1, s1s.at[0])
        sent(s2, s2s.at[0])
        ending = below.at[pl.ds(last * chips, chips)]

        @pl.when(source)
        def _():
            sent(below, bel_s.at[0])
            for delta in range(1, chips):
                sent(ending, bel_s.at[delta])

        @pl.when(passing)
        def _():
            sent(ending, bel_s.at[0])

        for s in range(last):
            @pl.when(x != source_x)
            def _():
                sent(outs.at[s], mov_s.at[s])

    def pieces_sent(s):
        if s == last:
            sent(cs.at[s, pl.ds(0, n - 1)], cs_s.at[s])
        else:
            @pl.when(home)
            def _():
                sent(cs.at[s, pl.ds(0, chips * n - 1)], cs_s.at[s])
        sent(sums.at[s, pl.ds(0, n - 1)], ag_s.at[s])

    diag_copy = pltpu.make_async_copy(diag_hbm, diag, in_sem.at[2 * supers])

    barrier = pltpu.get_barrier_semaphore()
    pl.semaphore_signal(barrier, inc=1, device_id=(mate, c), device_id_type=MESH)
    for near in (right, left):
        pl.semaphore_signal(barrier, inc=1, device_id=(r, near), device_id_type=MESH)
    for delta in range(1, chips):
        pl.semaphore_signal(barrier, inc=1, device_id=(((x + delta) % chips) * 2 + k, c), device_id_type=MESH)
    for s in range(supers):
        factor_copy(s).start()
        inverse_copy(s).start()
    for i in range(DEEP - 1):
        a_copy(i).start()
    diag_copy.start()
    factor_copy(0).wait()
    inverse_copy(0).wait()
    norm(0, 0)
    pl.semaphore_wait(barrier, chips + 2)
    ring(0, 1, 0, 0, c).start()
    norm(0, 1)
    ring(0, 1, 1, 0, c).start()
    for d in range(2):
        ring(0, 1, d, 1, c).start()
    for s in range(1, supers):
        factor_copy(s).wait()
        inverse_copy(s).wait()
    for g in range(1, chunks):
        for h in range(2):
            norm(g, h)
    for s in range(supers):
        @pl.loop(0, TILES)
        def _(m):
            kept[s, tile(m), :] = jnp.broadcast_to(coupled(s, c * rows + m * tall, tall), (tall, width))

    @pl.loop(0, steps)
    def _(i):
        g, j = i // n, i % n
        src = src_of(j)
        ahead, q = j // 2 + 1, j % 2

        @pl.when(ahead < n // 2)
        def _():
            for way in range(2):
                come = col_at((pos + (2 * way - 1) * ahead + n) % n)
                ring(g, ahead, way, q, come).wait_recv()

                @pl.when((ahead + 1 < n // 2) | (q == 0))
                def _():
                    ring(g, ahead + 1, way, q, come).start()

            for way in range(2):
                come = col_at((pos + (2 * way - 1) * ahead + n) % n)
                lend_half(g, come, q + way - 2 * q * way)

        @pl.when(((j == n - 4) | (j == n - 3)) & (g < chunks - 1))
        def _():
            for way in range(2):
                ring(g + 1, 1, way, q, c).start()

        @pl.when(j == n - 1)
        def _():
            for way in range(2):
                ring(g, n // 2, way, 0, src).wait_recv()
                lend_half(g, src, way)

        @pl.when(j == 0)
        def _():
            for h in range(2):
                lend_half(g, c, h)

        @pl.when((j == 0) | (j % 2 == 1))
        def _():
            lend(g, j)

        @pl.when((j < n - 1) & (j % 2 == 1))
        def _():
            lend(g, j + 1)

        @pl.when((i == steps - 1) & home)
        def _():
            for s in range(last):
                spread(s, 0)
                early_other(s)

        @pl.when((i >= LAG) & (i < steps - 2))
        def _():
            pass_below(i - LAG)

        @pl.when(i == steps - 2)
        def _():
            @pl.loop(steps - 2 - LAG, steps - 1 - NEAR)
            def _(late):
                pass_below(late)

        @pl.when(i == steps - 1)
        def _():
            pass_below(i - NEAR)

        a_copy(i).wait()

        @pl.when(i + DEEP - 1 < steps)
        def _():
            a_copy(i + DEEP - 1).start()

        @pl.loop(0, TILES)
        def _(m):
            term = jnp.dot(abuf[i % DEEP, tile(m), :], panel[g, src], preferred_element_type=jnp.float32)

            @pl.when(j == 0)
            def _():
                acc[g % 2, tile(m), :] = term

            @pl.when(j > 0)
            def _():
                acc[g % 2, tile(m), :] += term

            @pl.when(j == n - 1)
            def _():
                give(g, m)

        @pl.when((j >= BEGIN) & (j < BEGIN + TILES) & (g > 0) & (g <= chunks - supers))
        def _():
            send_across(g - 1, j - BEGIN)

        for s in range(last):
            own = chunks - supers + s

            @pl.when((j == 0) & (g == own + 1))
            def _():
                finish(own, s)

                @pl.when(x != source_x)
                def _():
                    move(s, x).start()

            @pl.when((j == 3) & (g == own + 1))
            def _():
                early_own(s)
    for i in range(steps - NEAR, steps - 1):
        pass_below(i)
    finish(chunks - 1, last)
    for s in range(last):
        early_send(s)
    gsum[...] = jnp.zeros_like(gsum)
    below_wait(last)
    below_arrived(last, 0, n - 1)
    correct(last, 0, n - 1, lambda at: outs[last, at, :])
    pass_below(steps - 1)
    below_arrived(last, n - 1, n)
    correct(last, n - 1, n, lambda at: outs[last, at, :])
    fill(last, 0)
    spread(last, 0)
    for s in range(last):
        collect(s)
    drain()
    diag_copy.wait()
    collect(last)
    for s in range(supers):
        update(s)
    for s in range(supers):
        pieces_sent(s)


def body(ancestor_order, factor_rows, factor_inverse, ancestor_inverse, diagonal_inverse):
    supers, piece, block = factor_rows.shape
    rows = ancestor_inverse.shape[0]
    row_count, n = lax.axis_size("row"), lax.axis_size("col")
    chips = row_count // 2
    depth = chips
    width = block // row_count
    pair = 2 * width
    chunks = supers * chips

    strips = piece % 128 != 0
    left = ancestor_inverse
    if strips:
        left = left.reshape(rows, n, piece).transpose(1, 0, 2)
    per_slab = rows // piece
    part = width // n
    half_type, full_type, dma = jnp.bfloat16, jnp.float32, pltpu.SemaphoreType.DMA
    anywhere = pl.BlockSpec(memory_space=pl.ANY)
    return pl.pallas_call(
        functools.partial(kernel, (chips, n, depth), strips),
        out_shape=(
            pltpu.VMEM((supers, rows, width), half_type),
            pltpu.VMEM((supers, block, width), full_type),
        ),
        in_specs=[pl.BlockSpec(memory_space=pltpu.VMEM)] + [anywhere] * 4,
        out_specs=(pl.BlockSpec(memory_space=pltpu.VMEM),) * 2,
        scratch_shapes=[
            pltpu.VMEM((supers, piece, block), half_type),
            pltpu.VMEM((supers, block, block), half_type),
            pltpu.VMEM((supers, block, width), full_type),
            pltpu.VMEM((chunks, n, piece, pair), half_type),
            pltpu.VMEM((DEEP, rows, piece), half_type),
            pltpu.VMEM((2, rows, pair), full_type),
            pltpu.VMEM((chunks, rows, width), half_type),
            pltpu.VMEM((chunks, rows, width), half_type),
            pltpu.VMEM((chunks - supers, rows, width), half_type),
            pltpu.VMEM((supers, chips, rows, width), half_type),
            pltpu.VMEM((supers, rows, width), full_type),
            pltpu.VMEM((max(supers - 1, 1), chips, rows, width), half_type),
            pltpu.VMEM((chunks, per_slab, piece, pair), half_type),
            pltpu.VMEM((supers, chips * n, part, block), half_type),
            pltpu.VMEM((supers, n, part, block), half_type),
            pltpu.VMEM((supers, 1, part, block), half_type),
            pltpu.VMEM((supers, n, part, block), half_type),
            pltpu.VMEM((width, block), full_type),
            dma((2 * supers + 1,)),
            dma((DEEP,)),
            dma((chunks,)),
            dma((2, 2, n // 2, 2)),
            dma((1,)),
            dma((chunks, TILES)),
            dma((1,)),
            dma((supers, chips)),
            dma((max(supers - 1, 1),)),
            dma((max(supers - 1, 1), chips)),
            dma((chips,)),
            dma((chunks, per_slab)),
            dma((chunks,)),
            dma((supers,)),
            dma((supers,)),
            dma((supers,)),
            dma((supers,)),
        ],
        compiler_params=pltpu.CompilerParams(
            collective_id=0, has_side_effects=True, vmem_limit_bytes=61 * 1024 * 1024
        ),
        cost_estimate=pl.CostEstimate(
            flops=2 * rows * n * piece * supers * block, bytes_accessed=8 * rows * n * piece, transcendentals=0
        ),
    )(ancestor_order, factor_rows, factor_inverse, diagonal_inverse, left)


def solution(mesh):
    placed = (P(), P(None, ("row", "col"), None), P(), P("col", "row"), P(None, None, "row"))
    return jax.shard_map(
        body,
        mesh=mesh,
        in_specs=placed,
        out_specs=(P(None, "col", "row"), P(None, None, "row")),
        check_vma=False,
    )
```

```python
import functools

import jax
import jax.numpy as jnp
from jax import lax
from jax.experimental import pallas as pl
from jax.experimental.pallas import tpu as pltpu
from jax.sharding import PartitionSpec as P

NSEL = 40
MESH = pl.DeviceIdType.MESH
TILES = 2
LAG = 6
NEAR = 2
BEGIN = 2
DEEP = 3


def kernel(
    dims, strips, order_ref, factor_hbm, inverse_hbm, diag_hbm, a_ref, outs, updated,
    factor, inverse, diag, panel, abuf, acc, s1, r1, s2, r2, kept, moved, below, cs, cr, total, sums, gsum,
    in_sem, a_sem, ring_s, ring_r, s1s, r1s, s2s, r2s, mov_s, mov_r, bel_s, bel_r, bel_l, cs_s, cs_r, ag_s, ag_r,
):
    chips, n, depth = dims
    supers, piece, block = factor.shape
    rows, pair = acc.shape[1], acc.shape[2]
    width = pair // 2
    chunks = supers * chips
    half = piece // 2
    cut = -(-half // 32) * 16
    tall = rows // TILES
    per_slab = rows // piece
    slabs = n // per_slab
    part = width // n
    r = lax.axis_index("row")
    c = lax.axis_index("col")
    x, k = r // 2, r % 2
    mate = x * 2 + 1 - k
    source_row = c // slabs
    source_x, source_k = source_row // 2, source_row % 2
    source = r == source_row
    passing = (k == source_k) & (x != source_x)
    home = x == source_x
    last = supers - 1
    length = n // depth
    steps = chunks * n

    def col_at(pos):
        y, i = pos // length, pos % length
        return (i + (y % 2) * (length - 1 - 2 * i)) * depth + y

    y, z = c % depth, c // depth
    pos = y * length + z + (y % 2) * (length - 1 - 2 * z)
    right, left = col_at((pos + 1) % n), col_at((pos + n - 1) % n)

    def src_of(j):
        t = (j + 1) // 2
        return col_at((pos + (1 - 2 * (j % 2)) * t + n) % n)

    def a_copy(i):
        src = src_of(i % n)
        if strips:
            view = a_ref.at[src]
        else:
            view = a_ref.at[:, pl.ds(pl.multiple_of(src * piece, piece), piece)]
        return pltpu.make_async_copy(view, abuf.at[i % DEEP], a_sem.at[i % DEEP])

    def block_of(g, at_x):
        return (at_x + 1 + g // supers) % chips

    def slot_of(g):
        return (g % supers) * chips + block_of(g, source_x)

    def ring(g, t, d, q, src):
        h = q + d - 2 * q * d
        view = panel.at[g, src, pl.ds(h * half, half)]
        return pltpu.make_async_remote_copy(
            src_ref=view, dst_ref=view,
            send_sem=ring_s.at[g], recv_sem=ring_r.at[d, g % 2, t - 1, q],
            device_id=(r, right * (1 - d) + left * d), device_id_type=MESH,
        )

    def ring_end(g, d, q, src):
        view = panel.at[g, src, pl.ds(end_at(d, q), (cut, half - cut)[q])]
        return pltpu.make_async_remote_copy(
            src_ref=view, dst_ref=view,
            send_sem=ring_s.at[g], recv_sem=ring_r.at[d, g % 2, n // 2 - 1, q],
            device_id=(r, right * (1 - d) + left * d), device_id_type=MESH,
        )

    def end_at(d, q):
        return d * half + q * cut

    def coupled(s, first, count):
        low = order_ref[pl.ds(s, 1), 0:NSEL] * block
        label = first + lax.broadcasted_iota(jnp.int32, (count, NSEL), 0)
        return jnp.sum(jnp.where((label >= low) & (label < low + block), 1.0, 0.0), axis=1, keepdims=True)

    def norm(g, h):
        s = g % supers
        keep = coupled(s, (r * n + c) * piece + h * half, half)
        at = pl.ds(pl.multiple_of(block_of(g, x) * pair, pair), pair)
        term = jnp.dot(factor[s, h * half:(h + 1) * half, :], inverse[s, :, at], preferred_element_type=jnp.float32)
        panel[g, c, h * half:(h + 1) * half, :] = (term * keep).astype(jnp.bfloat16)

    def below_copy(slot, at, src, to_row, sem):
        return pltpu.make_async_remote_copy(
            src_ref=src, dst_ref=below.at[slot, at], send_sem=sem, recv_sem=bel_r.at[slot, at],
            device_id=(to_row, c), device_id_type=MESH,
        )

    def below_here(slot, at, g, src):
        return pltpu.make_async_copy(panel.at[g, src], below.at[slot, at], bel_l.at[slot])

    def lend(g, j):
        src = src_of(j)
        slot, at = slot_of(g), src % per_slab

        @pl.when(source & (src // per_slab == c % slabs))
        def _():
            below_copy(slot, at, panel.at[g, src], mate, bel_s.at[0]).start()
            below_here(slot, at, g, src).start()

    def lend_part(g, src, first, count):
        slot, at = slot_of(g), src % per_slab
        view = pl.ds(first, count)

        @pl.when(source & (g % supers == last) & (src // per_slab == c % slabs))
        def _():
            for delta in range(1, chips):
                pltpu.make_async_remote_copy(
                    src_ref=panel.at[g, src, view], dst_ref=below.at[slot, at, view],
                    send_sem=bel_s.at[delta], recv_sem=bel_r.at[slot, at],
                    device_id=(((x + delta) % chips) * 2 + k, c), device_id_type=MESH,
                ).start()

    def pass_below(i):
        g, src = i // n, src_of(i % n)
        slot, at = slot_of(g), src % per_slab

        @pl.when(passing & (g % supers == last) & (src // per_slab == c % slabs))
        def _():
            copy = below_copy(slot, at, below.at[slot, at], mate, bel_s.at[0])
            copy.wait_recv()
            copy.start()

    def tile(m):
        return pl.ds(pl.multiple_of(m * tall, tall), tall)

    def mate_copy(g, m):
        return pltpu.make_async_remote_copy(
            src_ref=s1.at[g, tile(m)], dst_ref=r1.at[g, tile(m)],
            send_sem=s1s.at[0], recv_sem=r1s.at[g, m],
            device_id=(mate, c), device_id_type=MESH,
        )

    def cross_copy(g, m, slot):
        s = g % supers
        return pltpu.make_async_remote_copy(
            src_ref=s2.at[g, tile(m)], dst_ref=r2.at[s, slot, tile(m)],
            send_sem=s2s.at[0], recv_sem=r2s.at[s, slot],
            device_id=(block_of(g, x) * 2 + k, c), device_id_type=MESH,
        )

    def give(g, m):
        theirs = jnp.where(k == 0, acc[g % 2, tile(m), width:], acc[g % 2, tile(m), :width])
        s1[g, tile(m), :] = theirs.astype(jnp.bfloat16)
        mate_copy(g, m).start()

    def both(g, m):
        mate_copy(g, m).wait_recv()
        mine = jnp.where(k == 0, acc[g % 2, tile(m), :width], acc[g % 2, tile(m), width:])
        return mine + r1[g, tile(m), :].astype(jnp.float32)

    def send_across(g, m):
        s2[g, tile(m), :] = both(g, m).astype(jnp.bfloat16)
        cross_copy(g, m, x).start()

    def cross_wait(s, slot):
        pltpu.make_async_remote_copy(
            src_ref=s2.at[0], dst_ref=r2.at[s, slot], send_sem=s2s.at[0], recv_sem=r2s.at[s, slot],
            device_id=(mate, c), device_id_type=MESH,
        ).wait_recv()

    def finish_tile(g, s, m):
        whole = both(g, m)
        for delta in range(1, chips):
            whole += r2[s, (x + delta) % chips, tile(m), :].astype(jnp.float32)
        outs[s, tile(m), :] = (-(whole * kept[s, tile(m), :])).astype(jnp.bfloat16)

    def finish(g, s):
        for delta in range(1, chips):
            cross_wait(s, (x + delta) % chips)

        @pl.loop(0, TILES)
        def _(m):
            finish_tile(g, s, m)

    def move(s, slot):
        return pltpu.make_async_remote_copy(
            src_ref=outs.at[s], dst_ref=moved.at[s, slot], send_sem=mov_s.at[s], recv_sem=mov_r.at[s, slot],
            device_id=(source_x * 2 + k, c), device_id_type=MESH,
        )

    def piece_copy(s, first, count, slot, plane, to):
        return pltpu.make_async_remote_copy(
            src_ref=cs.at[s, pl.ds(first, count)], dst_ref=cr.at[s, pl.ds(slot, count)],
            send_sem=cs_s.at[s], recv_sem=cs_r.at[s],
            device_id=(plane * 2 + k, to), device_id_type=MESH,
        )

    def gather(s, slot, count, to):
        return pltpu.make_async_remote_copy(
            src_ref=total.at[s, pl.ds(0, count)], dst_ref=sums.at[s, pl.ds(slot, count)],
            send_sem=ag_s.at[s], recv_sem=ag_r.at[s],
            device_id=(r, to), device_id_type=MESH,
        )

    def below_wait(s):
        for e in range(chips):
            slot = slot_of(e * supers + s)

            @pl.when(source)
            def _():
                pltpu.make_async_copy(below.at[slot], below.at[slot], bel_l.at[slot]).wait()

    def correct(s, at, left_of):
        left = left_of(pl.ds(pl.multiple_of(at * piece, piece), piece))
        for b in range(chips):
            gsum[:, b * pair:(b + 1) * pair] -= lax.dot_general(
                left, below[s * chips + b, at], (((0,), (0,)), ((), ())), preferred_element_type=jnp.float32
            )

    def correct_all(s, left_of):
        @pl.loop(0, per_slab)
        def _(at):
            correct(s, at, left_of)

    def below_arrived(s, at):
        @pl.when(k != source_k)
        def _():
            for e in range(chips):
                slot = slot_of(e * supers + s)
                below_copy(slot, at, below.at[slot, at], mate, bel_s.at[0]).wait_recv()

    def finish_last():
        far = src_of(n - 1)
        own_far = far // per_slab == c % slabs
        per_tile = per_slab // TILES
        for delta in range(1, chips):
            cross_wait(last, (x + delta) % chips)
        below_wait(last)

        @pl.loop(0, TILES)
        def _(m):
            finish_tile(chunks - 1, last, m)

            @pl.loop(m * per_tile, (m + 1) * per_tile)
            def _(at):
                @pl.when((x == source_x) | (far // per_slab != c % slabs) | (at != far % per_slab))
                def _():
                    below_arrived(last, at)
                    correct(last, at, lambda rows_at: outs[last, rows_at, :])

        pass_below(steps - 1)

        @pl.when((x != source_x) & own_far)
        def _():
            below_arrived(last, far % per_slab)
            correct(last, far % per_slab, lambda rows_at: outs[last, rows_at, :])

    def farthest_first(send):
        for i in range(length):
            there = jnp.where(2 * z < length, length - 1 - i, i)
            for u in range(depth):
                to = there * depth + (y + 1 + u) % depth

                @pl.when(to != c)
                def _():
                    send(to)

    def fill(s, delta):
        for b in range(n):
            cs[s, delta * n + b] = gsum[b * part:(b + 1) * part, :].astype(jnp.bfloat16)
        if delta == 0:
            cr[s, c] = cs[s, c]

    def spread(s, delta):
        plane = (x + delta) % chips

        def send(to):
            piece_copy(s, delta * n + to, 1, c, plane, to).start()

        if delta:
            send(c)
        farthest_first(send)

    def early_own(s):
        @pl.when(home)
        def _():
            below_wait(s)
            for at in range(per_slab):
                below_arrived(s, at)
            gsum[...] = jnp.zeros_like(gsum)
            correct_all(s, lambda at: outs[s, at, :])
            fill(s, 0)

    def early_other(s):
        for delta in range(1, chips):
            plane = (x + delta) % chips
            move(s, plane).wait_recv()
            gsum[...] = jnp.zeros_like(gsum)
            correct_all(s, lambda at: moved[s, plane, at, :])
            fill(s, delta)

    def early_send(s):
        @pl.when(home)
        def _():
            for delta in range(1, chips):
                spread(s, delta)

    def collect(s):
        if s == last:
            piece_copy(s, 0, n - 1, 0, x, c).wait_recv()
        else:
            @pl.when(home)
            def _():
                piece_copy(s, 0, n - 1, 0, x, c).wait_recv()

            @pl.when(x != source_x)
            def _():
                piece_copy(s, 0, n, 0, x, c).wait_recv()
        summed = cr[s, 0].astype(jnp.float32)
        for b in range(1, n):
            summed += cr[s, b].astype(jnp.float32)
        total[s, 0] = summed.astype(jnp.bfloat16)
        farthest_first(lambda to: gather(s, c, 1, to).start())
        sums[s, c] = summed.astype(jnp.bfloat16)

    def update(s):
        pltpu.make_async_remote_copy(
            src_ref=sums.at[s, pl.ds(0, n - 1)], dst_ref=sums.at[s, pl.ds(0, n - 1)],
            send_sem=ag_s.at[s], recv_sem=ag_r.at[s], device_id=(mate, c), device_id_type=MESH,
        ).wait_recv()
        for b in range(n):
            gsum[b * part:(b + 1) * part, :] = sums[s, b].astype(jnp.float32)
        updated[s] = diag[s] + gsum[...].T

    def factor_copy(s):
        return pltpu.make_async_copy(factor_hbm.at[s], factor.at[s], in_sem.at[s])

    def inverse_copy(s):
        return pltpu.make_async_copy(inverse_hbm.at[s], inverse.at[s], in_sem.at[supers + s])

    def sent(ref, sem):
        pltpu.make_async_remote_copy(
            src_ref=ref, dst_ref=ref, send_sem=sem, recv_sem=sem, device_id=(mate, c), device_id_type=MESH
        ).wait_send()

    def drain():
        for g in range(chunks):
            sent(panel.at[g, pl.ds(0, n - 1)], ring_s.at[g])
        sent(s1, s1s.at[0])
        sent(s2, s2s.at[0])
        ending = below.at[pl.ds(last * chips, chips)]

        @pl.when(source)
        def _():
            sent(below, bel_s.at[0])
            for delta in range(1, chips):
                sent(ending, bel_s.at[delta])

        @pl.when(passing)
        def _():
            sent(ending, bel_s.at[0])

        for s in range(last):
            @pl.when(x != source_x)
            def _():
                sent(outs.at[s], mov_s.at[s])

    def pieces_sent(s):
        if s == last:
            sent(cs.at[s, pl.ds(0, n - 1)], cs_s.at[s])
        else:
            @pl.when(home)
            def _():
                sent(cs.at[s, pl.ds(0, chips * n - 1)], cs_s.at[s])
        sent(sums.at[s, pl.ds(0, n - 1)], ag_s.at[s])

    diag_copy = pltpu.make_async_copy(diag_hbm, diag, in_sem.at[2 * supers])

    factor_copy(0).start()
    inverse_copy(0).start()
    barrier = pltpu.get_barrier_semaphore()
    for near in (right, left):
        pl.semaphore_signal(barrier, inc=1, device_id=(r, near), device_id_type=MESH)
    pl.semaphore_signal(barrier, inc=1, device_id=(mate, c), device_id_type=MESH)
    for delta in range(1, chips):
        pl.semaphore_signal(barrier, inc=1, device_id=(((x + delta) % chips) * 2 + k, c), device_id_type=MESH)
    factor_copy(0).wait()
    inverse_copy(0).wait()
    norm(0, 0)
    pl.semaphore_wait(barrier, chips + 2)
    ring(0, 1, 0, 0, c).start()
    norm(0, 1)
    ring(0, 1, 1, 0, c).start()
    for d in range(2):
        ring(0, 1, d, 1, c).start()
    for s in range(1, supers):
        factor_copy(s).start()
        inverse_copy(s).start()
    for i in range(DEEP - 1):
        a_copy(i).start()
    diag_copy.start()
    for s in range(1, supers):
        factor_copy(s).wait()
        inverse_copy(s).wait()
    for g in range(1, chunks):
        for h in range(2):
            norm(g, h)
    for s in range(supers):
        @pl.loop(0, TILES)
        def _(m):
            kept[s, tile(m), :] = jnp.broadcast_to(coupled(s, c * rows + m * tall, tall), (tall, width))

    @pl.loop(0, steps)
    def _(i):
        g, j = i // n, i % n
        src = src_of(j)
        ahead, q = j // 2 + 1, j % 2

        @pl.when(ahead < n // 2)
        def _():
            for way in range(2):
                come = col_at((pos + (2 * way - 1) * ahead + n) % n)
                ring(g, ahead, way, q, come).wait_recv()

                @pl.when(ahead + 1 < n // 2)
                def _():
                    ring(g, ahead + 1, way, q, come).start()

                @pl.when((ahead + 1 == n // 2) & (q == 0))
                def _():
                    for e in range(2):
                        ring_end(g, way, e, come).start()

            for way in range(2):
                come = col_at((pos + (2 * way - 1) * ahead + n) % n)
                lend_part(g, come, pl.multiple_of((q + way - 2 * q * way) * half, half), half)

        @pl.when(((j == n - 4) | (j == n - 3)) & (g < chunks - 1))
        def _():
            for way in range(2):
                ring(g + 1, 1, way, q, c).start()

        far = src_of(n - 1)
        for e in range(2):
            @pl.when(j == n - 2 + e)
            def _():
                for way in range(2):
                    ring_end(g, way, e, far).wait_recv()
                    lend_part(g, far, end_at(way, e), (cut, half - cut)[e])

        @pl.when(j == 0)
        def _():
            for h in range(2):
                lend_part(g, c, h * half, half)

        @pl.when((j == 0) | (j % 2 == 1))
        def _():
            lend(g, j)

        @pl.when((j < n - 1) & (j % 2 == 1))
        def _():
            lend(g, j + 1)

        @pl.when((i == steps - 1) & home)
        def _():
            for s in range(last):
                spread(s, 0)
                early_other(s)
                early_send(s)

        @pl.when((i >= LAG) & (i < steps - 2))
        def _():
            pass_below(i - LAG)

        @pl.when(i == steps - 2)
        def _():
            @pl.loop(steps - 2 - LAG, steps - 1 - NEAR)
            def _(late):
                pass_below(late)

        @pl.when(i == steps - 1)
        def _():
            pass_below(i - NEAR)

        a_copy(i).wait()

        @pl.when(i + DEEP - 1 < steps)
        def _():
            a_copy(i + DEEP - 1).start()

        @pl.loop(0, TILES)
        def _(m):
            term = jnp.dot(abuf[i % DEEP, tile(m), :], panel[g, src], preferred_element_type=jnp.float32)

            @pl.when(j == 0)
            def _():
                acc[g % 2, tile(m), :] = term

            @pl.when(j > 0)
            def _():
                acc[g % 2, tile(m), :] += term

            @pl.when(j == n - 1)
            def _():
                give(g, m)

        @pl.when((j >= BEGIN) & (j < BEGIN + TILES) & (g > 0) & (g <= chunks - supers))
        def _():
            send_across(g - 1, j - BEGIN)

        for s in range(last):
            own = chunks - supers + s

            @pl.when((j == 0) & (g == own + 1))
            def _():
                finish(own, s)

                @pl.when(x != source_x)
                def _():
                    move(s, x).start()

            @pl.when((j == 3) & (g == own + 1))
            def _():
                early_own(s)
    for i in range(steps - NEAR, steps - 1):
        pass_below(i)
    gsum[...] = jnp.zeros_like(gsum)
    finish_last()
    fill(last, 0)
    spread(last, 0)
    for s in range(last):
        collect(s)
    drain()
    diag_copy.wait()
    collect(last)
    for s in range(supers):
        update(s)
    for s in range(supers):
        pieces_sent(s)


def store(outs, updated, out_hbm, updated_hbm, sem):
    copies = [pltpu.make_async_copy(a, b, sem.at[i]) for i, (a, b) in enumerate(((outs, out_hbm), (updated, updated_hbm)))]
    for copy in copies:
        copy.start()
    for copy in copies:
        copy.wait()


def body(ancestor_order, factor_rows, factor_inverse, ancestor_inverse, diagonal_inverse):
    supers, piece, block = factor_rows.shape
    rows = ancestor_inverse.shape[0]
    row_count, n = lax.axis_size("row"), lax.axis_size("col")
    chips = row_count // 2
    depth = chips
    width = block // row_count
    pair = 2 * width
    chunks = supers * chips

    strips = piece % 128 != 0
    left = ancestor_inverse
    if strips:
        left = left.reshape(rows, n, piece).transpose(1, 0, 2)
    per_slab = rows // piece
    part = width // n
    half_type, full_type, dma = jnp.bfloat16, jnp.float32, pltpu.SemaphoreType.DMA
    anywhere = pl.BlockSpec(memory_space=pl.ANY)
    shapes = (
        jax.ShapeDtypeStruct((supers, rows, width), half_type),
        jax.ShapeDtypeStruct((supers, block, width), full_type),
    )
    found = pl.pallas_call(
        functools.partial(kernel, (chips, n, depth), strips),
        out_shape=(
            pltpu.VMEM((supers, rows, width), half_type),
            pltpu.VMEM((supers, block, width), full_type),
        ),
        in_specs=[pl.BlockSpec(memory_space=pltpu.VMEM)] + [anywhere] * 4,
        out_specs=(pl.BlockSpec(memory_space=pltpu.VMEM),) * 2,
        scratch_shapes=[
            pltpu.VMEM((supers, piece, block), half_type),
            pltpu.VMEM((supers, block, block), half_type),
            pltpu.VMEM((supers, block, width), full_type),
            pltpu.VMEM((chunks, n, piece, pair), half_type),
            pltpu.VMEM((DEEP, rows, piece), half_type),
            pltpu.VMEM((2, rows, pair), full_type),
            pltpu.VMEM((chunks, rows, width), half_type),
            pltpu.VMEM((chunks, rows, width), half_type),
            pltpu.VMEM((chunks - supers, rows, width), half_type),
            pltpu.VMEM((supers, chips, rows, width), half_type),
            pltpu.VMEM((supers, rows, width), full_type),
            pltpu.VMEM((max(supers - 1, 1), chips, rows, width), half_type),
            pltpu.VMEM((chunks, per_slab, piece, pair), half_type),
            pltpu.VMEM((supers, chips * n, part, block), half_type),
            pltpu.VMEM((supers, n, part, block), half_type),
            pltpu.VMEM((supers, 1, part, block), half_type),
            pltpu.VMEM((supers, n, part, block), half_type),
            pltpu.VMEM((width, block), full_type),
            dma((2 * supers + 1,)),
            dma((DEEP,)),
            dma((chunks,)),
            dma((2, 2, n // 2, 2)),
            dma((1,)),
            dma((chunks, TILES)),
            dma((1,)),
            dma((supers, chips)),
            dma((max(supers - 1, 1),)),
            dma((max(supers - 1, 1), chips)),
            dma((chips,)),
            dma((chunks, per_slab)),
            dma((chunks,)),
            dma((supers,)),
            dma((supers,)),
            dma((supers,)),
            dma((supers,)),
        ],
        compiler_params=pltpu.CompilerParams(
            collective_id=0, has_side_effects=True, vmem_limit_bytes=61 * 1024 * 1024
        ),
        cost_estimate=pl.CostEstimate(
            flops=2 * rows * n * piece * supers * block, bytes_accessed=8 * rows * n * piece, transcendentals=0
        ),
    )(ancestor_order, factor_rows, factor_inverse, diagonal_inverse, left)
    return pl.pallas_call(
        store,
        out_shape=shapes,
        in_specs=[pl.BlockSpec(memory_space=pltpu.VMEM)] * 2,
        out_specs=(anywhere,) * 2,
        scratch_shapes=[dma((2,))],
        compiler_params=pltpu.CompilerParams(vmem_limit_bytes=1024 * 1024),
    )(*(pltpu.with_memory_space_constraint(one, pltpu.VMEM) for one in found))


def solution(mesh):
    placed = (P(), P(None, ("row", "col"), None), P(), P("col", "row"), P(None, None, "row"))
    return jax.shard_map(
        body,
        mesh=mesh,
        in_specs=placed,
        out_specs=(P(None, "col", "row"), P(None, None, "row")),
        check_vma=False,
    )
```

```python
import functools

import jax
import jax.numpy as jnp
from jax import lax
from jax.experimental import pallas as pl
from jax.experimental.pallas import tpu as pltpu
from jax.sharding import PartitionSpec as P

NSEL = 40
MESH = pl.DeviceIdType.MESH
TILES = 2
LAG = 6
NEAR = 2
BEGIN = 2
DEEP = 3


def kernel(
    dims, strips, order_hbm, factor_hbm, inverse_hbm, diag_hbm, a_ref, outs, updated,
    order_ref, factor, inverse, diag, panel, abuf, acc, s1, r1, s2, r2, kept, moved, below, cs, cr, total, sums, gsum,
    in_sem, a_sem, ring_s, ring_r, s1s, r1s, s2s, r2s, mov_s, mov_r, bel_s, bel_r, bel_l, cs_s, cs_r, ag_s, ag_r,
):
    chips, n, depth = dims
    supers, piece, block = factor.shape
    rows, pair = acc.shape[1], acc.shape[2]
    width = pair // 2
    chunks = supers * chips
    half = piece // 2
    cut = -(-half // 32) * 16
    tall = rows // TILES
    per_slab = rows // piece
    slabs = n // per_slab
    part = width // n
    r = lax.axis_index("row")
    c = lax.axis_index("col")
    x, k = r // 2, r % 2
    mate = x * 2 + 1 - k
    source_row = c // slabs
    source_x, source_k = source_row // 2, source_row % 2
    source = r == source_row
    passing = (k == source_k) & (x != source_x)
    home = x == source_x
    last = supers - 1
    length = n // depth
    steps = chunks * n

    def col_at(pos):
        y, i = pos // length, pos % length
        return (i + (y % 2) * (length - 1 - 2 * i)) * depth + y

    y, z = c % depth, c // depth
    pos = y * length + z + (y % 2) * (length - 1 - 2 * z)
    right, left = col_at((pos + 1) % n), col_at((pos + n - 1) % n)

    def src_of(j):
        t = (j + 1) // 2
        return col_at((pos + (1 - 2 * (j % 2)) * t + n) % n)

    def a_copy(i):
        src = src_of(i % n)
        if strips:
            view = a_ref.at[src]
        else:
            view = a_ref.at[:, pl.ds(pl.multiple_of(src * piece, piece), piece)]
        return pltpu.make_async_copy(view, abuf.at[i % DEEP], a_sem.at[i % DEEP])

    def block_of(g, at_x):
        return (at_x + 1 + g // supers) % chips

    def slot_of(g):
        return (g % supers) * chips + block_of(g, source_x)

    def ring(g, t, d, q, src):
        h = q + d - 2 * q * d
        view = panel.at[g, src, pl.ds(h * half, half)]
        return pltpu.make_async_remote_copy(
            src_ref=view, dst_ref=view,
            send_sem=ring_s.at[g], recv_sem=ring_r.at[d, t - 1, q],
            device_id=(r, right * (1 - d) + left * d), device_id_type=MESH,
        )

    def ring_end(g, d, q, src):
        view = panel.at[g, src, pl.ds(end_at(d, q), (cut, half - cut)[q])]
        return pltpu.make_async_remote_copy(
            src_ref=view, dst_ref=view,
            send_sem=ring_s.at[g], recv_sem=ring_r.at[d, n // 2 - 1, q],
            device_id=(r, right * (1 - d) + left * d), device_id_type=MESH,
        )

    def end_at(d, q):
        return d * half + q * cut

    def coupled(s, first, count):
        low = order_ref[pl.ds(s, 1), 0:NSEL] * block
        label = first + lax.broadcasted_iota(jnp.int32, (count, NSEL), 0)
        return jnp.sum(jnp.where((label >= low) & (label < low + block), 1.0, 0.0), axis=1, keepdims=True)

    def norm(g, h):
        s = g % supers
        keep = coupled(s, (r * n + c) * piece + h * half, half)
        at = pl.ds(pl.multiple_of(block_of(g, x) * pair, pair), pair)
        term = jnp.dot(factor[s, h * half:(h + 1) * half, :], inverse[s, :, at], preferred_element_type=jnp.float32)
        panel[g, c, h * half:(h + 1) * half, :] = (term * keep).astype(jnp.bfloat16)

    def below_copy(slot, at, src, to_row, sem):
        return pltpu.make_async_remote_copy(
            src_ref=src, dst_ref=below.at[slot, at], send_sem=sem, recv_sem=bel_r.at[slot, at],
            device_id=(to_row, c), device_id_type=MESH,
        )

    def below_here(slot, at, g, src):
        return pltpu.make_async_copy(panel.at[g, src], below.at[slot, at], bel_l.at[slot])

    def lend(g, j):
        src = src_of(j)
        slot, at = slot_of(g), src % per_slab

        @pl.when(source & (src // per_slab == c % slabs))
        def _():
            below_copy(slot, at, panel.at[g, src], mate, bel_s.at[0]).start()
            below_here(slot, at, g, src).start()

    def lend_part(g, src, first, count):
        slot, at = slot_of(g), src % per_slab
        view = pl.ds(first, count)

        @pl.when(source & (g % supers == last) & (src // per_slab == c % slabs))
        def _():
            for delta in range(1, chips):
                pltpu.make_async_remote_copy(
                    src_ref=panel.at[g, src, view], dst_ref=below.at[slot, at, view],
                    send_sem=bel_s.at[delta], recv_sem=bel_r.at[slot, at],
                    device_id=(((x + delta) % chips) * 2 + k, c), device_id_type=MESH,
                ).start()

    def pass_below(i):
        g, src = i // n, src_of(i % n)
        slot, at = slot_of(g), src % per_slab

        @pl.when(passing & (g % supers == last) & (src // per_slab == c % slabs))
        def _():
            copy = below_copy(slot, at, below.at[slot, at], mate, bel_s.at[0])
            copy.wait_recv()
            copy.start()

    def tile(m):
        return pl.ds(pl.multiple_of(m * tall, tall), tall)

    def mate_copy(g, m):
        return pltpu.make_async_remote_copy(
            src_ref=s1.at[g, tile(m)], dst_ref=r1.at[g, tile(m)],
            send_sem=s1s.at[0], recv_sem=r1s.at[g, m],
            device_id=(mate, c), device_id_type=MESH,
        )

    def cross_copy(g, m, slot):
        s = g % supers
        return pltpu.make_async_remote_copy(
            src_ref=s2.at[g, tile(m)], dst_ref=r2.at[s, slot, tile(m)],
            send_sem=s2s.at[0], recv_sem=r2s.at[s, slot],
            device_id=(block_of(g, x) * 2 + k, c), device_id_type=MESH,
        )

    def give(g, m):
        theirs = jnp.where(k == 0, acc[g % 2, tile(m), width:], acc[g % 2, tile(m), :width])
        s1[g, tile(m), :] = theirs.astype(jnp.bfloat16)
        mate_copy(g, m).start()

    def both(g, m):
        mate_copy(g, m).wait_recv()
        mine = jnp.where(k == 0, acc[g % 2, tile(m), :width], acc[g % 2, tile(m), width:])
        return mine + r1[g, tile(m), :].astype(jnp.float32)

    def send_across(g, m):
        s2[g, tile(m), :] = both(g, m).astype(jnp.bfloat16)
        cross_copy(g, m, x).start()

    def cross_wait(s, slot):
        pltpu.make_async_remote_copy(
            src_ref=s2.at[0], dst_ref=r2.at[s, slot], send_sem=s2s.at[0], recv_sem=r2s.at[s, slot],
            device_id=(mate, c), device_id_type=MESH,
        ).wait_recv()

    def finish_tile(g, s, m):
        whole = both(g, m)
        for delta in range(1, chips):
            whole += r2[s, (x + delta) % chips, tile(m), :].astype(jnp.float32)
        outs[s, tile(m), :] = (-(whole * kept[s, tile(m), :])).astype(jnp.bfloat16)

    def finish(g, s):
        for delta in range(1, chips):
            cross_wait(s, (x + delta) % chips)

        @pl.loop(0, TILES)
        def _(m):
            finish_tile(g, s, m)

    def move(s, slot):
        return pltpu.make_async_remote_copy(
            src_ref=outs.at[s], dst_ref=moved.at[s, slot], send_sem=mov_s.at[s], recv_sem=mov_r.at[s, slot],
            device_id=(source_x * 2 + k, c), device_id_type=MESH,
        )

    def piece_copy(s, first, count, slot, plane, to):
        return pltpu.make_async_remote_copy(
            src_ref=cs.at[s, pl.ds(first, count)], dst_ref=cr.at[s, pl.ds(slot, count)],
            send_sem=cs_s.at[s], recv_sem=cs_r.at[s],
            device_id=(plane * 2 + k, to), device_id_type=MESH,
        )

    def gather(s, slot, count, to):
        return pltpu.make_async_remote_copy(
            src_ref=total.at[s, pl.ds(0, count)], dst_ref=sums.at[s, pl.ds(slot, count)],
            send_sem=ag_s.at[s], recv_sem=ag_r.at[s],
            device_id=(r, to), device_id_type=MESH,
        )

    def below_wait(s):
        for e in range(chips):
            slot = slot_of(e * supers + s)

            @pl.when(source)
            def _():
                pltpu.make_async_copy(below.at[slot], below.at[slot], bel_l.at[slot]).wait()

    def correct(s, at, left_of):
        left = left_of(pl.ds(pl.multiple_of(at * piece, piece), piece))
        for b in range(chips):
            gsum[:, b * pair:(b + 1) * pair] -= lax.dot_general(
                left, below[s * chips + b, at], (((0,), (0,)), ((), ())), preferred_element_type=jnp.float32
            )

    def correct_all(s, left_of):
        @pl.loop(0, per_slab)
        def _(at):
            correct(s, at, left_of)

    def below_arrived(s, at):
        @pl.when(k != source_k)
        def _():
            for e in range(chips):
                slot = slot_of(e * supers + s)
                below_copy(slot, at, below.at[slot, at], mate, bel_s.at[0]).wait_recv()

    def finish_last():
        far = src_of(n - 1)
        own_far = far // per_slab == c % slabs
        per_tile = per_slab // TILES
        for delta in range(1, chips):
            cross_wait(last, (x + delta) % chips)
        below_wait(last)

        @pl.loop(0, TILES)
        def _(m):
            finish_tile(chunks - 1, last, m)

            @pl.loop(m * per_tile, (m + 1) * per_tile)
            def _(at):
                @pl.when((x == source_x) | (far // per_slab != c % slabs) | (at != far % per_slab))
                def _():
                    below_arrived(last, at)
                    correct(last, at, lambda rows_at: outs[last, rows_at, :])

        pass_below(steps - 1)

        @pl.when((x != source_x) & own_far)
        def _():
            below_arrived(last, far % per_slab)
            correct(last, far % per_slab, lambda rows_at: outs[last, rows_at, :])

    def farthest_first(send):
        for i in range(length):
            there = jnp.where(2 * z < length, length - 1 - i, i)
            for u in range(depth):
                to = there * depth + (y + 1 + u) % depth

                @pl.when(to != c)
                def _():
                    send(to)

    def fill(s, delta):
        for b in range(n):
            cs[s, delta * n + b] = gsum[b * part:(b + 1) * part, :].astype(jnp.bfloat16)
        if delta == 0:
            cr[s, c] = cs[s, c]

    def spread(s, delta):
        plane = (x + delta) % chips

        def send(to):
            piece_copy(s, delta * n + to, 1, c, plane, to).start()

        if delta:
            send(c)
        farthest_first(send)

    def early_own(s):
        @pl.when(home)
        def _():
            below_wait(s)
            for at in range(per_slab):
                below_arrived(s, at)
            gsum[...] = jnp.zeros_like(gsum)
            correct_all(s, lambda at: outs[s, at, :])
            fill(s, 0)

    def early_other(s):
        for delta in range(1, chips):
            plane = (x + delta) % chips
            move(s, plane).wait_recv()
            gsum[...] = jnp.zeros_like(gsum)
            correct_all(s, lambda at: moved[s, plane, at, :])
            fill(s, delta)

    def early_send(s):
        @pl.when(home)
        def _():
            for delta in range(1, chips):
                spread(s, delta)

    def collect(s):
        if s == last:
            piece_copy(s, 0, n - 1, 0, x, c).wait_recv()
        else:
            @pl.when(home)
            def _():
                piece_copy(s, 0, n - 1, 0, x, c).wait_recv()

            @pl.when(x != source_x)
            def _():
                piece_copy(s, 0, n, 0, x, c).wait_recv()
        summed = cr[s, 0].astype(jnp.float32)
        for b in range(1, n):
            summed += cr[s, b].astype(jnp.float32)
        total[s, 0] = summed.astype(jnp.bfloat16)
        farthest_first(lambda to: gather(s, c, 1, to).start())
        sums[s, c] = summed.astype(jnp.bfloat16)

    def update(s):
        pltpu.make_async_remote_copy(
            src_ref=sums.at[s, pl.ds(0, n - 1)], dst_ref=sums.at[s, pl.ds(0, n - 1)],
            send_sem=ag_s.at[s], recv_sem=ag_r.at[s], device_id=(mate, c), device_id_type=MESH,
        ).wait_recv()
        for b in range(n):
            gsum[b * part:(b + 1) * part, :] = sums[s, b].astype(jnp.float32)
        updated[s] = diag[s] + gsum[...].T

    def factor_copy(s):
        return pltpu.make_async_copy(factor_hbm.at[s], factor.at[s], in_sem.at[s])

    def first_factor(h):
        at = pl.ds(h * half, half)
        return pltpu.make_async_copy(factor_hbm.at[0, at], factor.at[0, at], in_sem.at[h * supers])

    def first_inverse(e):
        columns = pl.ds(pl.multiple_of(block_of(e * supers, x) * pair, pair), pair)
        return pltpu.make_async_copy(
            inverse_hbm.at[0, :, columns], inverse.at[0, :, columns], in_sem.at[2 * supers + 2 + e]
        )

    def inverse_copy(s):
        return pltpu.make_async_copy(inverse_hbm.at[s], inverse.at[s], in_sem.at[supers + s])

    def sent(ref, sem):
        pltpu.make_async_remote_copy(
            src_ref=ref, dst_ref=ref, send_sem=sem, recv_sem=sem, device_id=(mate, c), device_id_type=MESH
        ).wait_send()

    def drain():
        for g in range(chunks):
            sent(panel.at[g, pl.ds(0, n - 1)], ring_s.at[g])
        sent(s1, s1s.at[0])
        sent(s2, s2s.at[0])
        ending = below.at[pl.ds(last * chips, chips)]

        @pl.when(source)
        def _():
            sent(below, bel_s.at[0])
            for delta in range(1, chips):
                sent(ending, bel_s.at[delta])

        @pl.when(passing)
        def _():
            sent(ending, bel_s.at[0])

        for s in range(last):
            @pl.when(x != source_x)
            def _():
                sent(outs.at[s], mov_s.at[s])

    def pieces_sent(s):
        if s == last:
            sent(cs.at[s, pl.ds(0, n - 1)], cs_s.at[s])
        else:
            @pl.when(home)
            def _():
                sent(cs.at[s, pl.ds(0, chips * n - 1)], cs_s.at[s])
        sent(sums.at[s, pl.ds(0, n - 1)], ag_s.at[s])

    order_copy = pltpu.make_async_copy(order_hbm, order_ref, in_sem.at[2 * supers + 1])
    diag_copy = pltpu.make_async_copy(diag_hbm, diag, in_sem.at[2 * supers])

    for h in range(2):
        first_factor(h).start()
        if h == 0:
            first_inverse(0).start()
            order_copy.start()
    barrier = pltpu.get_barrier_semaphore()
    for near in (right, left):
        pl.semaphore_signal(barrier, inc=1, device_id=(r, near), device_id_type=MESH)
    pl.semaphore_signal(barrier, inc=1, device_id=(mate, c), device_id_type=MESH)
    for delta in range(1, chips):
        pl.semaphore_signal(barrier, inc=1, device_id=(((x + delta) % chips) * 2 + k, c), device_id_type=MESH)
    order_copy.wait()
    first_factor(0).wait()
    first_inverse(0).wait()
    norm(0, 0)
    pl.semaphore_wait(barrier, chips + 2)
    ring(0, 1, 0, 0, c).start()
    first_factor(1).wait()
    norm(0, 1)
    ring(0, 1, 1, 0, c).start()
    for d in range(2):
        ring(0, 1, d, 1, c).start()
    for e in range(1, chips):
        first_inverse(e).start()
    for s in range(1, supers):
        factor_copy(s).start()
        inverse_copy(s).start()
    for i in range(DEEP - 1):
        a_copy(i).start()
    diag_copy.start()
    for e in range(1, chips):
        first_inverse(e).wait()
    for s in range(1, supers):
        factor_copy(s).wait()
        inverse_copy(s).wait()
    for g in range(1, chunks):
        for h in range(2):
            norm(g, h)
    for s in range(supers):
        @pl.loop(0, TILES)
        def _(m):
            kept[s, tile(m), :] = jnp.broadcast_to(coupled(s, c * rows + m * tall, tall), (tall, width))

    @pl.loop(0, steps)
    def _(i):
        g, j = i // n, i % n
        src = src_of(j)
        ahead, q = j // 2 + 1, j % 2

        @pl.when(ahead < n // 2)
        def _():
            for way in range(2):
                come = col_at((pos + (2 * way - 1) * ahead + n) % n)
                ring(g, ahead, way, q, come).wait_recv()

                @pl.when(ahead + 1 < n // 2)
                def _():
                    ring(g, ahead + 1, way, q, come).start()

                @pl.when((ahead + 1 == n // 2) & (q == 0))
                def _():
                    for e in range(2):
                        ring_end(g, way, e, come).start()

            for way in range(2):
                come = col_at((pos + (2 * way - 1) * ahead + n) % n)
                lend_part(g, come, pl.multiple_of((q + way - 2 * q * way) * half, half), half)

        @pl.when(((j == n - 4) | (j == n - 3)) & (g < chunks - 1))
        def _():
            for way in range(2):
                ring(g + 1, 1, way, q, c).start()

        far = src_of(n - 1)
        for e in range(2):
            @pl.when(j == n - 2 + e)
            def _():
                for way in range(2):
                    ring_end(g, way, e, far).wait_recv()
                    lend_part(g, far, end_at(way, e), (cut, half - cut)[e])

        @pl.when(j == 0)
        def _():
            for h in range(2):
                lend_part(g, c, h * half, half)

        @pl.when((j == 0) | (j % 2 == 1))
        def _():
            lend(g, j)

        @pl.when((j < n - 1) & (j % 2 == 1))
        def _():
            lend(g, j + 1)

        @pl.when((i == steps - 1) & home)
        def _():
            for s in range(last):
                spread(s, 0)

        @pl.when((i >= LAG) & (i < steps - 2))
        def _():
            pass_below(i - LAG)

        @pl.when(i == steps - 2)
        def _():
            @pl.loop(steps - 2 - LAG, steps - 1 - NEAR)
            def _(late):
                pass_below(late)

        @pl.when(i == steps - 1)
        def _():
            pass_below(i - NEAR)

        a_copy(i).wait()

        @pl.when(i + DEEP - 1 < steps)
        def _():
            a_copy(i + DEEP - 1).start()

        @pl.loop(0, TILES)
        def _(m):
            term = jnp.dot(abuf[i % DEEP, tile(m), :], panel[g, src], preferred_element_type=jnp.float32)

            @pl.when(j == 0)
            def _():
                acc[g % 2, tile(m), :] = term

            @pl.when(j > 0)
            def _():
                acc[g % 2, tile(m), :] += term

            @pl.when(j == n - 1)
            def _():
                give(g, m)

        @pl.when((j >= BEGIN) & (j < BEGIN + TILES) & (g > 0) & (g <= chunks - supers))
        def _():
            send_across(g - 1, j - BEGIN)

        for s in range(last):
            own = chunks - supers + s

            @pl.when((j == 0) & (g == own + 1))
            def _():
                finish(own, s)

                @pl.when(x != source_x)
                def _():
                    move(s, x).start()

            @pl.when((j == 3) & (g == own + 1))
            def _():
                early_own(s)
    for i in range(steps - NEAR, steps - 1):
        pass_below(i)
    @pl.when(home)
    def _():
        for s in range(last):
            early_other(s)
            early_send(s)

    gsum[...] = jnp.zeros_like(gsum)
    finish_last()
    fill(last, 0)
    spread(last, 0)
    for s in range(last):
        collect(s)
    drain()
    diag_copy.wait()
    collect(last)
    for s in range(supers):
        update(s)
    for s in range(supers):
        pieces_sent(s)


def store(outs, updated, out_hbm, updated_hbm, sem):
    copies = [pltpu.make_async_copy(a, b, sem.at[i]) for i, (a, b) in enumerate(((outs, out_hbm), (updated, updated_hbm)))]
    for copy in copies:
        copy.start()
    for copy in copies:
        copy.wait()


def body(ancestor_order, factor_rows, factor_inverse, ancestor_inverse, diagonal_inverse):
    supers, piece, block = factor_rows.shape
    rows = ancestor_inverse.shape[0]
    row_count, n = lax.axis_size("row"), lax.axis_size("col")
    chips = row_count // 2
    depth = chips
    width = block // row_count
    pair = 2 * width
    chunks = supers * chips

    strips = piece % 128 != 0
    left = ancestor_inverse
    if strips:
        left = left.reshape(rows, n, piece).transpose(1, 0, 2)
    per_slab = rows // piece
    part = width // n
    half_type, full_type, dma = jnp.bfloat16, jnp.float32, pltpu.SemaphoreType.DMA
    anywhere = pl.BlockSpec(memory_space=pl.ANY)
    shapes = (
        jax.ShapeDtypeStruct((supers, rows, width), half_type),
        jax.ShapeDtypeStruct((supers, block, width), full_type),
    )
    found = pl.pallas_call(
        functools.partial(kernel, (chips, n, depth), strips),
        out_shape=(
            pltpu.VMEM((supers, rows, width), half_type),
            pltpu.VMEM((supers, block, width), full_type),
        ),
        in_specs=[anywhere] * 5,
        out_specs=(pl.BlockSpec(memory_space=pltpu.VMEM),) * 2,
        scratch_shapes=[
            pltpu.VMEM(ancestor_order.shape, ancestor_order.dtype),
            pltpu.VMEM((supers, piece, block), half_type),
            pltpu.VMEM((supers, block, block), half_type),
            pltpu.VMEM((supers, block, width), full_type),
            pltpu.VMEM((chunks, n, piece, pair), half_type),
            pltpu.VMEM((DEEP, rows, piece), half_type),
            pltpu.VMEM((2, rows, pair), full_type),
            pltpu.VMEM((chunks, rows, width), half_type),
            pltpu.VMEM((chunks, rows, width), half_type),
            pltpu.VMEM((chunks - supers, rows, width), half_type),
            pltpu.VMEM((supers, chips, rows, width), half_type),
            pltpu.VMEM((supers, rows, width), full_type),
            pltpu.VMEM((max(supers - 1, 1), chips, rows, width), half_type),
            pltpu.VMEM((chunks, per_slab, piece, pair), half_type),
            pltpu.VMEM((supers, chips * n, part, block), half_type),
            pltpu.VMEM((supers, n, part, block), half_type),
            pltpu.VMEM((supers, 1, part, block), half_type),
            pltpu.VMEM((supers, n, part, block), half_type),
            pltpu.VMEM((width, block), full_type),
            dma((2 * supers + 2 + chips,)),
            dma((DEEP,)),
            dma((chunks,)),
            dma((2, n // 2, 2)),
            dma((1,)),
            dma((chunks, TILES)),
            dma((1,)),
            dma((supers, chips)),
            dma((max(supers - 1, 1),)),
            dma((max(supers - 1, 1), chips)),
            dma((chips,)),
            dma((chunks, per_slab)),
            dma((chunks,)),
            dma((supers,)),
            dma((supers,)),
            dma((supers,)),
            dma((supers,)),
        ],
        compiler_params=pltpu.CompilerParams(
            collective_id=0, has_side_effects=True, vmem_limit_bytes=61 * 1024 * 1024
        ),
        cost_estimate=pl.CostEstimate(
            flops=2 * rows * n * piece * supers * block, bytes_accessed=8 * rows * n * piece, transcendentals=0
        ),
    )(ancestor_order, factor_rows, factor_inverse, diagonal_inverse, left)
    return pl.pallas_call(
        store,
        out_shape=shapes,
        in_specs=[pl.BlockSpec(memory_space=pltpu.VMEM)] * 2,
        out_specs=(anywhere,) * 2,
        scratch_shapes=[dma((2,))],
        compiler_params=pltpu.CompilerParams(vmem_limit_bytes=1024 * 1024),
    )(*(pltpu.with_memory_space_constraint(one, pltpu.VMEM) for one in found))


def solution(mesh):
    placed = (P(), P(None, ("row", "col"), None), P(), P("col", "row"), P(None, None, "row"))
    return jax.shard_map(
        body,
        mesh=mesh,
        in_specs=placed,
        out_specs=(P(None, "col", "row"), P(None, None, "row")),
        check_vma=False,
    )
```

```python
import functools

import jax
import jax.numpy as jnp
from jax import lax
from jax.experimental import pallas as pl
from jax.experimental.pallas import tpu as pltpu
from jax.sharding import PartitionSpec as P

NSEL = 40
MESH = pl.DeviceIdType.MESH
TILES = 2
LAG = 6
NEAR = 2
BEGIN = 2
DEEP = 3


def kernel(
    dims, strips, order_hbm, factor_hbm, inverse_hbm, diag_hbm, a_ref, outs, updated,
    order_ref, factor, inverse, diag, panel, abuf, acc, s1, r1, s2, r2, kept, moved, below, cs, cr, total, sums, gsum,
    in_sem, a_sem, ring_s, ring_r, s1s, r1s, s2s, r2s, mov_s, mov_r, bel_s, bel_r, bel_e, bel_l, cs_s, cs_r, ag_s, ag_r,
):
    chips, n, depth = dims
    supers, piece, block = factor.shape
    rows, pair = acc.shape[1], acc.shape[2]
    width = pair // 2
    chunks = supers * chips
    half = piece // 2
    cut = -(-half // 32) * 16
    tall = rows // TILES
    per_slab = rows // piece
    slabs = n // per_slab
    part = width // n
    r = lax.axis_index("row")
    c = lax.axis_index("col")
    x, k = r // 2, r % 2
    mate = x * 2 + 1 - k
    source_row = c // slabs
    source_x, source_k = source_row // 2, source_row % 2
    source = r == source_row
    passing = (k == source_k) & (x != source_x)
    home = x == source_x
    last = supers - 1
    length = n // depth
    steps = chunks * n

    def col_at(pos):
        y, i = pos // length, pos % length
        return (i + (y % 2) * (length - 1 - 2 * i)) * depth + y

    y, z = c % depth, c // depth
    pos = y * length + z + (y % 2) * (length - 1 - 2 * z)
    right, left = col_at((pos + 1) % n), col_at((pos + n - 1) % n)

    def src_of(j):
        t = (j + 1) // 2
        return col_at((pos + (1 - 2 * (j % 2)) * t + n) % n)

    def a_copy(i):
        src = src_of(i % n)
        if strips:
            view = a_ref.at[src]
        else:
            view = a_ref.at[:, pl.ds(pl.multiple_of(src * piece, piece), piece)]
        return pltpu.make_async_copy(view, abuf.at[i % DEEP], a_sem.at[i % DEEP])

    def block_of(g, at_x):
        return (at_x + 1 + g // supers) % chips

    def slot_of(g):
        return (g % supers) * chips + block_of(g, source_x)

    def ring(g, t, d, q, src):
        h = q + d - 2 * q * d
        view = panel.at[g, src, pl.ds(h * half, half)]
        return pltpu.make_async_remote_copy(
            src_ref=view, dst_ref=view,
            send_sem=ring_s.at[g], recv_sem=ring_r.at[d, t - 1, q],
            device_id=(r, right * (1 - d) + left * d), device_id_type=MESH,
        )

    def ring_end(g, d, q, src):
        view = panel.at[g, src, pl.ds(end_at(d, q), (cut, half - cut)[q])]
        return pltpu.make_async_remote_copy(
            src_ref=view, dst_ref=view,
            send_sem=ring_s.at[g], recv_sem=ring_r.at[d, n // 2 - 1, q],
            device_id=(r, right * (1 - d) + left * d), device_id_type=MESH,
        )

    def end_at(d, q):
        return d * half + q * cut

    def coupled(s, first, count):
        low = order_ref[pl.ds(s, 1), 0:NSEL] * block
        label = first + lax.broadcasted_iota(jnp.int32, (count, NSEL), 0)
        return jnp.sum(jnp.where((label >= low) & (label < low + block), 1.0, 0.0), axis=1, keepdims=True)

    def norm(g, h):
        s = g % supers
        keep = coupled(s, (r * n + c) * piece + h * half, half)
        at = pl.ds(pl.multiple_of(block_of(g, x) * pair, pair), pair)
        term = jnp.dot(factor[s, h * half:(h + 1) * half, :], inverse[s, :, at], preferred_element_type=jnp.float32)
        panel[g, c, h * half:(h + 1) * half, :] = (term * keep).astype(jnp.bfloat16)

    def below_copy(slot, at, src, to_row, sem):
        return pltpu.make_async_remote_copy(
            src_ref=src, dst_ref=below.at[slot, at], send_sem=sem, recv_sem=bel_r.at[slot, at],
            device_id=(to_row, c), device_id_type=MESH,
        )

    def below_here(slot, at, g, src):
        return pltpu.make_async_copy(panel.at[g, src], below.at[slot, at], bel_l.at[slot])

    def lend(g, j):
        src = src_of(j)
        slot, at = slot_of(g), src % per_slab

        @pl.when(source & (src // per_slab == c % slabs))
        def _():
            below_copy(slot, at, panel.at[g, src], mate, bel_s.at[0]).start()
            below_here(slot, at, g, src).start()

    def lend_part(g, src, first, count, sem=None):
        slot, at = slot_of(g), src % per_slab
        view = pl.ds(first, count)
        sem = bel_r.at[slot, at] if sem is None else sem

        @pl.when(source & (g % supers == last) & (src // per_slab == c % slabs))
        def _():
            for delta in range(1, chips):
                pltpu.make_async_remote_copy(
                    src_ref=panel.at[g, src, view], dst_ref=below.at[slot, at, view],
                    send_sem=bel_s.at[delta], recv_sem=sem,
                    device_id=(((x + delta) % chips) * 2 + k, c), device_id_type=MESH,
                ).start()

    def pass_below(i):
        g, src = i // n, src_of(i % n)
        slot, at = slot_of(g), src % per_slab

        @pl.when(passing & (g % supers == last) & (src // per_slab == c % slabs))
        def _():
            copy = below_copy(slot, at, below.at[slot, at], mate, bel_s.at[0])
            copy.wait_recv()
            copy.start()

    def pass_far(e):
        far, count = src_of(n - 1), (cut, half - cut)[e]
        slot, at = slot_of(chunks - 1), far % per_slab

        @pl.when(passing & (far // per_slab == c % slabs))
        def _():
            both_ways = below.at[slot, at, pl.ds(0, 2 * count)]
            pltpu.make_async_remote_copy(
                src_ref=both_ways, dst_ref=both_ways, send_sem=bel_s.at[0], recv_sem=bel_e.at[e],
                device_id=(mate, c), device_id_type=MESH,
            ).wait_recv()
            for way in range(2):
                view = below.at[slot, at, pl.ds(end_at(way, e), count)]
                pltpu.make_async_remote_copy(
                    src_ref=view, dst_ref=view, send_sem=bel_s.at[0], recv_sem=bel_r.at[slot, at],
                    device_id=(mate, c), device_id_type=MESH,
                ).start()

    def tile(m):
        return pl.ds(pl.multiple_of(m * tall, tall), tall)

    def mate_copy(g, m):
        return pltpu.make_async_remote_copy(
            src_ref=s1.at[g, tile(m)], dst_ref=r1.at[g, tile(m)],
            send_sem=s1s.at[0], recv_sem=r1s.at[g, m],
            device_id=(mate, c), device_id_type=MESH,
        )

    def cross_copy(g, m, slot):
        s = g % supers
        return pltpu.make_async_remote_copy(
            src_ref=s2.at[g, tile(m)], dst_ref=r2.at[s, slot, tile(m)],
            send_sem=s2s.at[0], recv_sem=r2s.at[s, slot],
            device_id=(block_of(g, x) * 2 + k, c), device_id_type=MESH,
        )

    def give(g, m):
        theirs = jnp.where(k == 0, acc[g % 2, tile(m), width:], acc[g % 2, tile(m), :width])
        s1[g, tile(m), :] = theirs.astype(jnp.bfloat16)
        mate_copy(g, m).start()

    def both(g, m):
        mate_copy(g, m).wait_recv()
        mine = jnp.where(k == 0, acc[g % 2, tile(m), :width], acc[g % 2, tile(m), width:])
        return mine + r1[g, tile(m), :].astype(jnp.float32)

    def send_across(g, m):
        s2[g, tile(m), :] = both(g, m).astype(jnp.bfloat16)
        cross_copy(g, m, x).start()

    def cross_wait(s, slot):
        pltpu.make_async_remote_copy(
            src_ref=s2.at[0], dst_ref=r2.at[s, slot], send_sem=s2s.at[0], recv_sem=r2s.at[s, slot],
            device_id=(mate, c), device_id_type=MESH,
        ).wait_recv()

    def finish_tile(g, s, m):
        whole = both(g, m)
        for delta in range(1, chips):
            whole += r2[s, (x + delta) % chips, tile(m), :].astype(jnp.float32)
        outs[s, tile(m), :] = (-(whole * kept[s, tile(m), :])).astype(jnp.bfloat16)

    def finish(g, s):
        for delta in range(1, chips):
            cross_wait(s, (x + delta) % chips)

        @pl.loop(0, TILES)
        def _(m):
            finish_tile(g, s, m)

    def move(s, slot):
        return pltpu.make_async_remote_copy(
            src_ref=outs.at[s], dst_ref=moved.at[s, slot], send_sem=mov_s.at[s], recv_sem=mov_r.at[s, slot],
            device_id=(source_x * 2 + k, c), device_id_type=MESH,
        )

    def piece_copy(s, first, count, slot, plane, to):
        return pltpu.make_async_remote_copy(
            src_ref=cs.at[s, pl.ds(first, count)], dst_ref=cr.at[s, pl.ds(slot, count)],
            send_sem=cs_s.at[s], recv_sem=cs_r.at[s],
            device_id=(plane * 2 + k, to), device_id_type=MESH,
        )

    def gather(s, slot, count, to):
        return pltpu.make_async_remote_copy(
            src_ref=total.at[s, pl.ds(0, count)], dst_ref=sums.at[s, pl.ds(slot, count)],
            send_sem=ag_s.at[s], recv_sem=ag_r.at[s],
            device_id=(r, to), device_id_type=MESH,
        )

    def below_wait(s):
        for e in range(chips):
            slot = slot_of(e * supers + s)

            @pl.when(source)
            def _():
                pltpu.make_async_copy(below.at[slot], below.at[slot], bel_l.at[slot]).wait()

    def correct(s, at, left_of):
        left = left_of(pl.ds(pl.multiple_of(at * piece, piece), piece))
        for b in range(chips):
            gsum[:, b * pair:(b + 1) * pair] -= lax.dot_general(
                left, below[s * chips + b, at], (((0,), (0,)), ((), ())), preferred_element_type=jnp.float32
            )

    def correct_all(s, left_of):
        @pl.loop(0, per_slab)
        def _(at):
            correct(s, at, left_of)

    def below_arrived(s, at):
        @pl.when(k != source_k)
        def _():
            for e in range(chips):
                slot = slot_of(e * supers + s)
                below_copy(slot, at, below.at[slot, at], mate, bel_s.at[0]).wait_recv()

    def finish_last():
        far = src_of(n - 1)
        own_far = far // per_slab == c % slabs
        per_tile = per_slab // TILES
        for delta in range(1, chips):
            cross_wait(last, (x + delta) % chips)
        below_wait(last)

        @pl.loop(0, TILES)
        def _(m):
            finish_tile(chunks - 1, last, m)

            @pl.loop(m * per_tile, (m + 1) * per_tile)
            def _(at):
                @pl.when((x == source_x) | (far // per_slab != c % slabs) | (at != far % per_slab))
                def _():
                    below_arrived(last, at)
                    correct(last, at, lambda rows_at: outs[last, rows_at, :])

        pass_far(1)

        @pl.when((x != source_x) & own_far)
        def _():
            below_arrived(last, far % per_slab)
            correct(last, far % per_slab, lambda rows_at: outs[last, rows_at, :])

    def farthest_first(send):
        for i in range(length):
            there = jnp.where(2 * z < length, length - 1 - i, i)
            for u in range(depth):
                to = there * depth + (y + 1 + u) % depth

                @pl.when(to != c)
                def _():
                    send(to)

    def fill(s, delta):
        for b in range(n):
            cs[s, delta * n + b] = gsum[b * part:(b + 1) * part, :].astype(jnp.bfloat16)
        if delta == 0:
            cr[s, c] = cs[s, c]

    def spread(s, delta):
        plane = (x + delta) % chips

        def send(to):
            piece_copy(s, delta * n + to, 1, c, plane, to).start()

        if delta:
            send(c)
        farthest_first(send)

    def early_own(s):
        @pl.when(home)
        def _():
            below_wait(s)
            for at in range(per_slab):
                below_arrived(s, at)
            gsum[...] = jnp.zeros_like(gsum)
            correct_all(s, lambda at: outs[s, at, :])
            fill(s, 0)

    def early_other(s):
        for delta in range(1, chips):
            plane = (x + delta) % chips
            move(s, plane).wait_recv()
            gsum[...] = jnp.zeros_like(gsum)
            correct_all(s, lambda at: moved[s, plane, at, :])
            fill(s, delta)

    def early_send(s):
        @pl.when(home)
        def _():
            for delta in range(1, chips):
                spread(s, delta)

    def collect(s):
        if s == last:
            piece_copy(s, 0, n - 1, 0, x, c).wait_recv()
        else:
            @pl.when(home)
            def _():
                piece_copy(s, 0, n - 1, 0, x, c).wait_recv()

            @pl.when(x != source_x)
            def _():
                piece_copy(s, 0, n, 0, x, c).wait_recv()
        summed = cr[s, 0].astype(jnp.float32)
        for b in range(1, n):
            summed += cr[s, b].astype(jnp.float32)
        total[s, 0] = summed.astype(jnp.bfloat16)
        farthest_first(lambda to: gather(s, c, 1, to).start())
        sums[s, c] = summed.astype(jnp.bfloat16)

    def update(s):
        pltpu.make_async_remote_copy(
            src_ref=sums.at[s, pl.ds(0, n - 1)], dst_ref=sums.at[s, pl.ds(0, n - 1)],
            send_sem=ag_s.at[s], recv_sem=ag_r.at[s], device_id=(mate, c), device_id_type=MESH,
        ).wait_recv()
        for b in range(n):
            gsum[b * part:(b + 1) * part, :] = sums[s, b].astype(jnp.float32)
        updated[s] = diag[s] + gsum[...].T

    def factor_copy(s):
        return pltpu.make_async_copy(factor_hbm.at[s], factor.at[s], in_sem.at[s])

    def first_factor(h):
        at = pl.ds(h * half, half)
        return pltpu.make_async_copy(factor_hbm.at[0, at], factor.at[0, at], in_sem.at[h * supers])

    def first_inverse(e):
        columns = pl.ds(pl.multiple_of(block_of(e * supers, x) * pair, pair), pair)
        return pltpu.make_async_copy(
            inverse_hbm.at[0, :, columns], inverse.at[0, :, columns], in_sem.at[2 * supers + 2 + e]
        )

    def inverse_copy(s):
        return pltpu.make_async_copy(inverse_hbm.at[s], inverse.at[s], in_sem.at[supers + s])

    def sent(ref, sem):
        pltpu.make_async_remote_copy(
            src_ref=ref, dst_ref=ref, send_sem=sem, recv_sem=sem, device_id=(mate, c), device_id_type=MESH
        ).wait_send()

    def drain():
        for g in range(chunks):
            sent(panel.at[g, pl.ds(0, n - 1)], ring_s.at[g])
        sent(s1, s1s.at[0])
        sent(s2, s2s.at[0])
        ending = below.at[pl.ds(last * chips, chips)]

        @pl.when(source)
        def _():
            sent(below, bel_s.at[0])
            for delta in range(1, chips):
                sent(ending, bel_s.at[delta])

        @pl.when(passing)
        def _():
            sent(ending, bel_s.at[0])

        for s in range(last):
            @pl.when(x != source_x)
            def _():
                sent(outs.at[s], mov_s.at[s])

    def pieces_sent(s):
        if s == last:
            sent(cs.at[s, pl.ds(0, n - 1)], cs_s.at[s])
        else:
            @pl.when(home)
            def _():
                sent(cs.at[s, pl.ds(0, chips * n - 1)], cs_s.at[s])
        sent(sums.at[s, pl.ds(0, n - 1)], ag_s.at[s])

    order_copy = pltpu.make_async_copy(order_hbm, order_ref, in_sem.at[2 * supers + 1])
    diag_copy = pltpu.make_async_copy(diag_hbm, diag, in_sem.at[2 * supers])

    for h in range(2):
        first_factor(h).start()
        if h == 0:
            first_inverse(0).start()
            order_copy.start()
    barrier = pltpu.get_barrier_semaphore()
    for near in (right, left):
        pl.semaphore_signal(barrier, inc=1, device_id=(r, near), device_id_type=MESH)
    pl.semaphore_signal(barrier, inc=1, device_id=(mate, c), device_id_type=MESH)
    for delta in range(1, chips):
        pl.semaphore_signal(barrier, inc=1, device_id=(((x + delta) % chips) * 2 + k, c), device_id_type=MESH)
    order_copy.wait()
    first_factor(0).wait()
    first_inverse(0).wait()
    norm(0, 0)
    pl.semaphore_wait(barrier, chips + 2)
    ring(0, 1, 0, 0, c).start()
    first_factor(1).wait()
    norm(0, 1)
    ring(0, 1, 1, 0, c).start()
    for d in range(2):
        ring(0, 1, d, 1, c).start()
    for e in range(1, chips):
        first_inverse(e).start()
    for s in range(1, supers):
        factor_copy(s).start()
        inverse_copy(s).start()
    for i in range(DEEP - 1):
        a_copy(i).start()
    diag_copy.start()
    for e in range(1, chips):
        first_inverse(e).wait()
    for s in range(1, supers):
        factor_copy(s).wait()
        inverse_copy(s).wait()
    for g in range(1, chunks):
        for h in range(2):
            norm(g, h)
    for s in range(supers):
        @pl.loop(0, TILES)
        def _(m):
            kept[s, tile(m), :] = jnp.broadcast_to(coupled(s, c * rows + m * tall, tall), (tall, width))

    @pl.loop(0, steps)
    def _(i):
        g, j = i // n, i % n
        src = src_of(j)
        ahead, q = j // 2 + 1, j % 2

        @pl.when(ahead < n // 2)
        def _():
            for way in range(2):
                come = col_at((pos + (2 * way - 1) * ahead + n) % n)
                ring(g, ahead, way, q, come).wait_recv()

                @pl.when(ahead + 1 < n // 2)
                def _():
                    ring(g, ahead + 1, way, q, come).start()

                @pl.when((ahead + 1 == n // 2) & (q == 0))
                def _():
                    for e in range(2):
                        ring_end(g, way, e, come).start()

            for way in range(2):
                come = col_at((pos + (2 * way - 1) * ahead + n) % n)
                lend_part(g, come, pl.multiple_of((q + way - 2 * q * way) * half, half), half)

        @pl.when(((j == n - 4) | (j == n - 3)) & (g < chunks - 1))
        def _():
            for way in range(2):
                ring(g + 1, 1, way, q, c).start()

        far = src_of(n - 1)
        for e in range(2):
            @pl.when(j == n - 2 + e)
            def _():
                for way in range(2):
                    ring_end(g, way, e, far).wait_recv()

                    @pl.when(g < chunks - 1)
                    def _():
                        lend_part(g, far, end_at(way, e), (cut, half - cut)[e])

                    @pl.when(g == chunks - 1)
                    def _():
                        lend_part(g, far, end_at(way, e), (cut, half - cut)[e], bel_e.at[e])

        @pl.when(j == 0)
        def _():
            for h in range(2):
                lend_part(g, c, h * half, half)

        @pl.when((j == 0) | (j % 2 == 1))
        def _():
            lend(g, j)

        @pl.when((j < n - 1) & (j % 2 == 1))
        def _():
            lend(g, j + 1)

        @pl.when((i == steps - 2) & home)
        def _():
            for s in range(last):
                spread(s, 0)

        @pl.when((i >= LAG) & (i < steps - 2))
        def _():
            pass_below(i - LAG)

        @pl.when(i == steps - 2)
        def _():
            @pl.loop(steps - 2 - LAG, steps - 1 - NEAR)
            def _(late):
                pass_below(late)

        @pl.when(i == steps - 1)
        def _():
            pass_below(i - NEAR)

        a_copy(i).wait()

        @pl.when(i + DEEP - 1 < steps)
        def _():
            a_copy(i + DEEP - 1).start()

        @pl.when(j == 0)
        def _():
            acc[g % 2] = jnp.dot(abuf[i % DEEP], panel[g, src], preferred_element_type=jnp.float32)

        @pl.when((j > 0) & (j < n - 1))
        def _():
            acc[g % 2] += jnp.dot(abuf[i % DEEP], panel[g, src], preferred_element_type=jnp.float32)

        @pl.when(j == n - 1)
        def _():
            @pl.loop(0, TILES)
            def _(m):
                acc[g % 2, tile(m), :] += jnp.dot(
                    abuf[i % DEEP, tile(m), :], panel[g, src], preferred_element_type=jnp.float32
                )
                give(g, m)

        @pl.when((j >= BEGIN) & (j < BEGIN + TILES) & (g > 0) & (g <= chunks - supers))
        def _():
            send_across(g - 1, j - BEGIN)

        for s in range(last):
            own = chunks - supers + s

            @pl.when((j == 0) & (g == own + 1))
            def _():
                finish(own, s)

                @pl.when(x != source_x)
                def _():
                    move(s, x).start()

            @pl.when((j == 3) & (g == own + 1))
            def _():
                early_own(s)
    for i in range(steps - NEAR, steps - 1):
        pass_below(i)
    @pl.when(home)
    def _():
        for s in range(last):
            early_other(s)
            early_send(s)

    gsum[...] = jnp.zeros_like(gsum)
    pass_far(0)
    finish_last()
    fill(last, 0)
    spread(last, 0)
    for s in range(last):
        collect(s)
    drain()
    diag_copy.wait()
    collect(last)
    for s in range(supers):
        update(s)
    for s in range(supers):
        pieces_sent(s)


def store(outs, updated, out_hbm, updated_hbm, sem):
    copies = [pltpu.make_async_copy(a, b, sem.at[i]) for i, (a, b) in enumerate(((outs, out_hbm), (updated, updated_hbm)))]
    for copy in copies:
        copy.start()
    for copy in copies:
        copy.wait()


def body(ancestor_order, factor_rows, factor_inverse, ancestor_inverse, diagonal_inverse):
    supers, piece, block = factor_rows.shape
    rows = ancestor_inverse.shape[0]
    row_count, n = lax.axis_size("row"), lax.axis_size("col")
    chips = row_count // 2
    depth = chips
    width = block // row_count
    pair = 2 * width
    chunks = supers * chips

    strips = piece % 128 != 0
    left = ancestor_inverse
    if strips:
        left = left.reshape(rows, n, piece).transpose(1, 0, 2)
    per_slab = rows // piece
    part = width // n
    half_type, full_type, dma = jnp.bfloat16, jnp.float32, pltpu.SemaphoreType.DMA
    anywhere = pl.BlockSpec(memory_space=pl.ANY)
    shapes = (
        jax.ShapeDtypeStruct((supers, rows, width), half_type),
        jax.ShapeDtypeStruct((supers, block, width), full_type),
    )
    found = pl.pallas_call(
        functools.partial(kernel, (chips, n, depth), strips),
        out_shape=(
            pltpu.VMEM((supers, rows, width), half_type),
            pltpu.VMEM((supers, block, width), full_type),
        ),
        in_specs=[anywhere] * 5,
        out_specs=(pl.BlockSpec(memory_space=pltpu.VMEM),) * 2,
        scratch_shapes=[
            pltpu.VMEM(ancestor_order.shape, ancestor_order.dtype),
            pltpu.VMEM((supers, piece, block), half_type),
            pltpu.VMEM((supers, block, block), half_type),
            pltpu.VMEM((supers, block, width), full_type),
            pltpu.VMEM((chunks, n, piece, pair), half_type),
            pltpu.VMEM((DEEP, rows, piece), half_type),
            pltpu.VMEM((2, rows, pair), full_type),
            pltpu.VMEM((chunks, rows, width), half_type),
            pltpu.VMEM((chunks, rows, width), half_type),
            pltpu.VMEM((chunks - supers, rows, width), half_type),
            pltpu.VMEM((supers, chips, rows, width), half_type),
            pltpu.VMEM((supers, rows, width), full_type),
            pltpu.VMEM((max(supers - 1, 1), chips, rows, width), half_type),
            pltpu.VMEM((chunks, per_slab, piece, pair), half_type),
            pltpu.VMEM((supers, chips * n, part, block), half_type),
            pltpu.VMEM((supers, n, part, block), half_type),
            pltpu.VMEM((supers, 1, part, block), half_type),
            pltpu.VMEM((supers, n, part, block), half_type),
            pltpu.VMEM((width, block), full_type),
            dma((2 * supers + 2 + chips,)),
            dma((DEEP,)),
            dma((chunks,)),
            dma((2, n // 2, 2)),
            dma((1,)),
            dma((chunks, TILES)),
            dma((1,)),
            dma((supers, chips)),
            dma((max(supers - 1, 1),)),
            dma((max(supers - 1, 1), chips)),
            dma((chips,)),
            dma((chunks, per_slab)),
            dma((2,)),
            dma((chunks,)),
            dma((supers,)),
            dma((supers,)),
            dma((supers,)),
            dma((supers,)),
        ],
        compiler_params=pltpu.CompilerParams(
            collective_id=0, has_side_effects=True, vmem_limit_bytes=61 * 1024 * 1024
        ),
        cost_estimate=pl.CostEstimate(
            flops=2 * rows * n * piece * supers * block, bytes_accessed=8 * rows * n * piece, transcendentals=0
        ),
    )(ancestor_order, factor_rows, factor_inverse, diagonal_inverse, left)
    return pl.pallas_call(
        store,
        out_shape=shapes,
        in_specs=[pl.BlockSpec(memory_space=pltpu.VMEM)] * 2,
        out_specs=(anywhere,) * 2,
        scratch_shapes=[dma((2,))],
        compiler_params=pltpu.CompilerParams(vmem_limit_bytes=1024 * 1024),
    )(*(pltpu.with_memory_space_constraint(one, pltpu.VMEM) for one in found))


def solution(mesh):
    placed = (P(), P(None, ("row", "col"), None), P(), P("col", "row"), P(None, None, "row"))
    return jax.shard_map(
        body,
        mesh=mesh,
        in_specs=placed,
        out_specs=(P(None, "col", "row"), P(None, None, "row")),
        check_vma=False,
    )
```
